256 devices in a mesh: dp: 32 (over y, z), group: 8 (over x, core).
Axes of the slice: x: 4, y: 4, z: 8, core: 2. Of those that a mesh axis runs over, the one named last changes fastest.
Arguments:
- rewards: bfloat16 [65536, 4096], P(('dp', 'group')), may hold values from -6 to 6
- values: bfloat16 [65536, 4096], P(('dp', 'group')), may hold values from -6 to 6
- lengths: int32 [65536], P(('dp', 'group')), may hold values from 1 to 4096
- decay_rate: float32 [65536], P(('dp', 'group')), may hold values from 3.8146973e-06 to 0.03125
- piece_dest: int32 [32, 32], P('dp'), may hold values from 0 to 31, each once within a row
- row_perm: int32 [512, 128], P(('dp', 'group')), may hold values from 0 to 127, each once within a row
- minibatch: int32 [65536], P(('dp', 'group')), may hold values from 0 to 63
Outputs:
- white_rewards: bfloat16 [65536, 4096], P(('dp', 'group'))
- white_advantage: bfloat16 [65536, 4096], P(('dp', 'group'))
The draws below stay inside these ranges and needn't reach their ends.
Inputs may be any that keep to these rules, and one draw needn't show every extreme that they name: Each row of piece_dest names every index of dp once. Each row of row_perm names every number below 128 once.
All inputs are finite; a program needn't handle non-finite values.
Results may differ from the reference program's by a relative error of at most 0.0049.
Values may be sent and summed in bfloat16 or wider, within the bound.
A program may use at most 64 MiB of HBM per device.

```python
import math
import jax
import jax.numpy as jnp
from jax import lax

LEN = 4096
BLK = 128
ROWS_DEV = 256
MINIBATCHES = 64
ROWS = 65536
BLOCKS = 512
N_DP = 32
N_GROUP = 8


def plant(result, rng, least, high):
    shape = result.shape
    index_at = [jax.random.randint(jax.random.fold_in(rng, axis), (), 0, shape[axis]) for axis in range(len(shape))]
    result = result.at[tuple(index_at)].set(least)
    longest = shape.index(max(shape))
    index_at[longest] = (index_at[longest] + 1) % shape[longest]
    return result.at[tuple(index_at)].set(high)


def shard_levels(rng, dims, pieces, least, high):
    gain, own = 1.0, jax.random.fold_in(rng, 6)
    for dim, blocks in pieces:
        heights = jnp.exp(jax.random.uniform(jax.random.fold_in(own, dim), (blocks,), jnp.float32, least / len(pieces), high / len(pieces)))
        gain = gain * jnp.repeat(heights, dims[dim] // blocks).reshape([-1 if axis == dim else 1 for axis in range(len(dims))])
    return gain


def centred(key, extent, scale, most, pieces=(), kind=jnp.bfloat16):
    entries = scale * jax.random.normal(key, extent, jnp.float32)
    if pieces:
        entries = entries * shard_levels(key, extent, pieces, -0.22, 0.18)
    return jnp.clip(entries, -most, most).astype(kind)


def setup_inputs(seed: int = 0) -> dict:
    streams_of = jax.random.split(jax.random.key(seed), 8)
    return {
        "rewards": centred(streams_of[0], (ROWS, LEN), 1.0, 6.0, ((0, 256),)),
        "values": centred(streams_of[1], (ROWS, LEN), 1.0, 6.0, ((0, 256),)),
        "lengths": plant(jax.random.randint(streams_of[2], (ROWS,), 1, LEN + 1), jax.random.fold_in(streams_of[2], 1), 1, LEN).astype(jnp.int32),
        "decay_rate": jnp.clip(jnp.exp(math.log(0.03125) - 9.010913 * jax.random.uniform(streams_of[3], (ROWS,), jnp.float32) ** shard_levels(streams_of[3], (ROWS,), ((0, 256),), -0.2, 0.2)), 3.814697265625e-06, 0.03125),
        "piece_dest": jax.vmap(lambda own: jax.random.permutation(own, N_DP))(jax.random.split(streams_of[4], N_DP)).reshape((N_DP, N_DP)).astype(jnp.int32),
        "row_perm": jax.vmap(lambda own: jax.random.permutation(own, BLK))(jax.random.split(streams_of[5], BLOCKS)).reshape((BLOCKS, BLK)).astype(jnp.int32),
        "minibatch": plant(jax.random.randint(streams_of[6], (ROWS,), 0, MINIBATCHES), jax.random.fold_in(streams_of[6], 1), 0, MINIBATCHES - 1).astype(jnp.int32),
    }


def reference(rewards, values, lengths, decay_rate, piece_dest, row_perm, minibatch):
    rows_all, span_all = rewards.shape
    position = jnp.arange(span_all, dtype=jnp.int32)
    is_valid = position[None, :] < lengths[:, None]
    next_valid = position[None, :] + 1 < lengths[:, None]
    per_step = jnp.exp(-decay_rate)
    value_f = values.astype(jnp.float32)
    value_next = jnp.concatenate([value_f[:, 1:], jnp.zeros((rows_all, 1), jnp.float32)], axis=1)
    td_error = rewards.astype(jnp.float32) + per_step[:, None] * jnp.where(next_valid, value_next, 0.0) - value_f
    td_error = jnp.where(is_valid, td_error, 0.0)

    def backward(carry, column):
        fresh = column + per_step * carry
        return (fresh, fresh)
    starting = jnp.zeros((rows_all,), jnp.float32)
    final_carry, stacked = lax.scan(backward, starting, td_error.T, reverse=True)
    advantage = stacked.T.astype(jnp.bfloat16)
    piece = ROWS_DEV // N_DP
    source_slot = jnp.argsort(piece_dest, axis=1).astype(jnp.int32)
    out_rows = jnp.arange(rows_all, dtype=jnp.int32)
    device = out_rows // ROWS_DEV
    target = device // N_GROUP
    column_group = device % N_GROUP
    inside = out_rows % ROWS_DEV
    chosen = inside // BLK * BLK + row_perm.reshape(-1).astype(jnp.int32)
    source_dev = chosen // piece
    within = chosen % piece
    source_row = (source_dev * N_GROUP + column_group) * ROWS_DEV + source_slot[source_dev, target] * piece + within
    moved_rewards = jnp.take(rewards, source_row, axis=0).astype(jnp.float32)
    moved_advantage = jnp.take(advantage, source_row, axis=0).astype(jnp.float32)
    moved_lengths = jnp.take(lengths, source_row, axis=0)
    valid = position[None, :] < moved_lengths[:, None]
    moved_rewards = jnp.where(valid, moved_rewards, 0.0)
    moved_advantage = jnp.where(valid, moved_advantage, 0.0)
    count = jax.ops.segment_sum(moved_lengths.astype(jnp.float32), minibatch, num_segments=MINIBATCHES)
    count = jnp.maximum(count, 1.0)

    def whiten(moved):
        mean = jax.ops.segment_sum(lax.optimization_barrier(jnp.sum(moved, axis=1)), minibatch, num_segments=MINIBATCHES) / count
        deviation = jnp.where(valid, moved - mean[minibatch][:, None], 0.0)
        spread = jax.ops.segment_sum(lax.optimization_barrier(jnp.sum(deviation * deviation, axis=1)), minibatch, num_segments=MINIBATCHES) / count
        return (deviation / jnp.sqrt(spread[minibatch][:, None] + 1e-05)).astype(jnp.bfloat16)
    return (whiten(moved_rewards), whiten(moved_advantage))
```

```python
import functools

import jax
import jax.numpy as jnp
from jax import lax
from jax.experimental import pallas as pl
from jax.experimental.pallas import tpu as pltpu
from jax.sharding import PartitionSpec as P

MESH = pl.DeviceIdType.MESH
HIGHEST = lax.Precision.HIGHEST
F32 = jnp.float32
BF16 = jnp.bfloat16
LANES = 128
NZ = 8


def dot(a, b, dims=(((1,), (0,)), ((), ())), precision=None):
    return lax.dot_general(a, b, dims, precision=precision, preferred_element_type=F32)


def iota(shape, dim):
    return lax.broadcasted_iota(jnp.int32, shape, dim)


def column(row):
    on = iota((LANES, LANES), 0) == iota((LANES, LANES), 1)
    return jnp.sum(jnp.where(on, row, 0.0), axis=1, keepdims=True)


def kernel(
    cfg, slots_ref, smalls_ref, r_hbm, v_hbm, out_r, out_a,
    rbuf, vbuf, send_r, send_a, vals, recv_r, recv_a,
    cols, scales, sums, chooser, member, stats, tsend, trecv, part, st_z, st_y, st_g,
    load_sem, bulk_send, bulk_recv, t_send, t_recv, g_send, g_recv, z_send, z_recv, y_send, y_recv,
):
    n_dp, n_group, piece, span, width = cfg
    rows = n_dp * piece
    n_y = n_dp // NZ
    me = lax.axis_index("dp")
    group = lax.axis_index("group")
    y, z = me // NZ, lax.rem(me, NZ)
    waves = 2 * span // width
    half = waves // 2

    def peer(k):
        return lax.rem(y + k // NZ, n_y) * NZ + lax.rem(z + lax.rem(k, NZ), NZ)

    load_r = pltpu.make_async_copy(r_hbm, rbuf, load_sem.at[0])
    load_v = pltpu.make_async_copy(v_hbm, vbuf, load_sem.at[1])
    load_r.start()
    load_v.start()

    barrier = pltpu.get_barrier_semaphore()

    def greet(k, c):
        pl.semaphore_signal(barrier, 1, device_id={"dp": peer(k)}, device_id_type=MESH)
        return c

    lax.fori_loop(1, n_dp, greet, 0)

    def greet_group(k, c):
        pl.semaphore_signal(
            barrier, 1, device_id={"group": lax.rem(group + k, n_group)}, device_id_type=MESH
        )
        return c

    lax.fori_loop(1, n_group, greet_group, 0)

    for b in range(2):
        for q in range(2):
            spread = jnp.broadcast_to(
                column(smalls_ref[2 * q + b : 2 * q + b + 1, :]), (LANES, LANES)
            )
            per = LANES // piece
            cols[q, per * b : per * (b + 1)] = spread.reshape(per, piece, LANES)

    load_r.wait()

    def gather_r(d, c):
        p = slots_ref[d]
        send_r[d] = rbuf[p]
        sums[0, d] = cols[0, p]
        sums[1, d] = cols[1, p]
        return c

    lax.fori_loop(0, n_dp, gather_r, 0)

    pl.semaphore_wait(barrier, n_dp - 1 + n_group - 1)

    def bulk(w, k):
        source, target = (send_r, recv_r) if w < half else (send_a, recv_a)
        lanes = pl.ds((w % half) * width, width)
        return pltpu.make_async_remote_copy(
            source.at[peer(k), :, lanes], target.at[me, :, lanes],
            bulk_send.at[w, k], bulk_recv.at[w, k],
            device_id={"dp": peer(k)}, device_id_type=MESH,
        )

    def start_wave(w):
        def go(k, c):
            bulk(w, k).start()
            return c

        lax.fori_loop(1, n_dp, go, 0)

    start_wave(0)

    load_v.wait()

    def gather_v(d, c):
        vals[d] = vbuf[slots_ref[d]]
        return c

    lax.fori_loop(0, n_dp, gather_v, 0)
    recv_r[me] = send_r[me]

    lane = iota((rows, LANES), 1)
    lane_f = lane.astype(F32)
    lengths = sums[0].reshape(rows, LANES).astype(jnp.int32)
    rate = sums[1].reshape(rows, LANES)
    cols[0] = sums[0]
    scales[0] = jnp.exp(-rate)
    scales[1] = jnp.exp(-rate * lane_f)
    scales[2] = jnp.exp(rate * lane_f)
    scales[3] = jnp.exp(-rate * (LANES - lane_f))
    sums[...] = jnp.zeros_like(sums)
    triangle = (iota((LANES, LANES), 0) >= iota((LANES, LANES), 1)).astype(F32)

    def block(i, carry):
        next_head, next_value = carry
        at = span // LANES - 1 - i
        lanes = pl.ds(pl.multiple_of(at * LANES, LANES), LANES)
        position = at * LANES + lane
        length = cols[0].reshape(rows, LANES).astype(jnp.int32)
        reward = send_r[:, :, lanes].astype(F32).reshape(rows, LANES)
        value = vals[:, :, lanes].astype(F32).reshape(rows, LANES)
        valid = position < length
        value_next = jnp.where(lane == LANES - 1, next_value, pltpu.roll(value, LANES - 1, 1))
        value_next = jnp.where(position + 1 < length, value_next, 0.0)
        td = jnp.where(valid, reward + scales[0] * value_next - value, 0.0)
        local = dot(td * scales[1], triangle, precision=HIGHEST) * scales[2]
        total = local + scales[3] * next_head
        rounded = jnp.where(valid, total, 0.0).astype(BF16)
        send_a[:, :, lanes] = rounded.reshape(n_dp, piece, LANES)
        reward = jnp.where(valid, reward, 0.0)
        kept = rounded.astype(F32)
        for q, term in enumerate((reward, kept, reward * reward, kept * kept)):
            sums[q] += term.reshape(n_dp, piece, LANES)
        return total[:, 0:1], value[:, 0:1]

    zero = jnp.zeros((rows, 1), F32)
    lax.fori_loop(0, span // LANES, block, (zero, zero))
    recv_a[me] = send_a[me]

    term_of, row_of = lane // piece, lax.rem(lane, piece)
    own = row_of == lax.rem(iota((rows, LANES), 0), piece)
    packed = jnp.where(own & (term_of == 0), cols[0].reshape(rows, LANES), 0.0)
    for q in range(4):
        total = jnp.sum(sums[q].reshape(rows, LANES), axis=1, keepdims=True)
        packed = jnp.where(own & (term_of == q + 1), total, packed)
    tsend[...] = jnp.sum(packed.reshape(n_dp, piece, LANES), axis=1, keepdims=True)

    for b in range(2):
        here = slice(b * LANES, (b + 1) * LANES)
        order = column(smalls_ref[6 + b : 7 + b, :]).astype(jnp.int32)
        chooser[b] = (order == iota((LANES, LANES), 1)).astype(BF16)
        batch = column(smalls_ref[4 + b : 5 + b, :]).astype(jnp.int32)
        member[here] = (batch == iota((LANES, LANES), 1)).astype(F32)

    def terms(k):
        return pltpu.make_async_remote_copy(
            tsend.at[peer(k)], trecv.at[me], t_send.at[k], t_recv.at[k],
            device_id={"dp": peer(k)}, device_id_type=MESH,
        )

    def terms_go(k, c):
        terms(k).start()
        return c

    def terms_wait(k, c):
        terms(k).wait()
        return c

    lax.fori_loop(1, n_dp, terms_go, 0)
    start_wave(1)
    trecv[me] = tsend[me]
    lax.fori_loop(1, n_dp, terms_wait, 0)

    spread = jnp.broadcast_to(trecv[...], (n_dp, piece, LANES)).reshape(rows, LANES)
    spread = jnp.where(own, spread, 0.0)
    select = (iota((LANES, LANES), 0) // piece == iota((LANES, LANES), 1)).astype(F32)
    totals = jnp.zeros((LANES, LANES), F32)
    for b in range(2):
        here = slice(b * LANES, (b + 1) * LANES)
        moved = dot(chooser[b].astype(F32), spread[here], precision=HIGHEST)
        moved = dot(moved, select, precision=HIGHEST)
        stats[4, here] = jnp.broadcast_to(moved[:, 0:1], (LANES, LANES))
        totals += dot(moved, member[here], (((0,), (0,)), ((), ())), precision=HIGHEST)

    def exchange(store, index, sizes, target, send_sem, recv_sem, between):
        store[index] = part[...]

        def copy(k):
            return pltpu.make_async_remote_copy(
                part, store.at[index], send_sem.at[k], recv_sem.at[k],
                device_id=target(k), device_id_type=MESH,
            )

        def go(k, c):
            copy(k).start()
            return c

        def done(k, c):
            copy(k).wait()
            return c

        lax.fori_loop(1, sizes, go, 0)
        between()
        lax.fori_loop(1, sizes, done, 0)
        part[...] = jnp.sum(store[...], axis=0)

    part[...] = totals[0:8]
    exchange(
        st_g, group, n_group, lambda k: {"group": lax.rem(group + k, n_group)},
        g_send, g_recv, lambda: None,
    )
    exchange(
        st_z, z, NZ, lambda k: {"dp": y * NZ + lax.rem(z + k, NZ)},
        z_send, z_recv, lambda: start_wave(2),
    )
    exchange(
        st_y, y, n_y, lambda k: {"dp": lax.rem(y + k, n_y) * NZ + z},
        y_send, y_recv, lambda: start_wave(3),
    )

    total = part[...]
    count = jnp.maximum(total[0:1], 1.0)
    for q in range(2):
        mean = total[1 + q : 2 + q] / count
        spread = total[3 + q : 4 + q] / count - mean * mean
        for s, value in enumerate((mean, lax.rsqrt(spread + 1e-05))):
            picked = jnp.sum(member[...] * value, axis=1, keepdims=True)
            stats[2 * q + s] = jnp.broadcast_to(picked, (rows, LANES))

    tile = 256
    for w in range(waves):
        def wait_wave(k, c):
            bulk(w, k).wait()
            return c

        lax.fori_loop(1, n_dp, wait_wave, 0)
        q = 0 if w < half else 1
        source, out = ((recv_r, out_r), (recv_a, out_a))[q]

        def finish(i, c):
            start = pl.multiple_of((w % half) * width + i * tile, LANES)
            for b in range(2):
                per = LANES // piece
                block = source[per * b : per * (b + 1), :, pl.ds(start, tile)]
                block = block.astype(F32).reshape(LANES, tile).astype(BF16)
                moved = dot(chooser[b], block)
                here = slice(b * LANES, (b + 1) * LANES)
                length = stats[4, here].astype(jnp.int32)
                for s in range(tile // LANES):
                    position = start + s * LANES + iota((LANES, LANES), 1)
                    white = (moved[:, s * LANES : (s + 1) * LANES] - stats[2 * q, here]) * stats[
                        2 * q + 1, here
                    ]
                    out[here, pl.ds(start + s * LANES, LANES)] = jnp.where(
                        position < length, white, 0.0
                    ).astype(BF16)
            return c

        lax.fori_loop(0, width // tile, finish, 0)


def local(rewards, values, lengths, decay_rate, piece_dest, row_perm, minibatch, *, n_dp, n_group):
    rows, span = rewards.shape
    piece = rows // n_dp
    width = span // 2
    slots = jnp.sum(
        jnp.where(
            piece_dest[0][None, :] == jnp.arange(n_dp, dtype=jnp.int32)[:, None],
            jnp.arange(n_dp, dtype=jnp.int32)[None, :],
            0,
        ),
        axis=1,
    )
    smalls = jnp.concatenate(
        [
            lengths.astype(F32).reshape(2, LANES),
            decay_rate.reshape(2, LANES),
            minibatch.astype(F32).reshape(2, LANES),
            row_perm.astype(F32),
        ],
        axis=0,
    )
    vmem = pl.BlockSpec(memory_space=pltpu.VMEM)
    hbm = pl.BlockSpec(memory_space=pl.ANY)
    bulk = pltpu.VMEM((n_dp, piece, span), BF16)
    dma = pltpu.SemaphoreType.DMA
    waves = 2 * span // width
    n_y = n_dp // NZ
    return pl.pallas_call(
        functools.partial(kernel, (n_dp, n_group, piece, span, width)),
        out_shape=(jax.ShapeDtypeStruct((rows, span), BF16),) * 2,
        in_specs=[pl.BlockSpec(memory_space=pltpu.SMEM), vmem, hbm, hbm],
        out_specs=(vmem, vmem),
        scratch_shapes=[bulk] * 7
        + [
            pltpu.VMEM((2, n_dp, piece, LANES), F32),
            pltpu.VMEM((4, rows, LANES), F32),
            pltpu.VMEM((4, n_dp, piece, LANES), F32),
            pltpu.VMEM((2, LANES, LANES), BF16),
            pltpu.VMEM((rows, LANES), F32),
            pltpu.VMEM((5, rows, LANES), F32),
            pltpu.VMEM((n_dp, 1, LANES), F32),
            pltpu.VMEM((n_dp, 1, LANES), F32),
            pltpu.VMEM((8, LANES), F32),
            pltpu.VMEM((NZ, 8, LANES), F32),
            pltpu.VMEM((n_y, 8, LANES), F32),
            pltpu.VMEM((n_group, 8, LANES), F32),
            dma((2,)),
            dma((waves, n_dp)), dma((waves, n_dp)),
            dma((n_dp,)), dma((n_dp,)),
            dma((n_group,)), dma((n_group,)),
            dma((NZ,)), dma((NZ,)),
            dma((n_y,)), dma((n_y,)),
        ],
        compiler_params=pltpu.CompilerParams(
            collective_id=0, has_side_effects=True, vmem_limit_bytes=40 * 2**20
        ),
        name="reshuffle",
    )(
        slots,
        smalls,
        rewards.reshape(n_dp, piece, span),
        values.reshape(n_dp, piece, span),
    )


def solution(mesh):
    both = ("dp", "group")
    return jax.shard_map(
        functools.partial(local, n_dp=mesh.shape["dp"], n_group=mesh.shape["group"]),
        mesh=mesh,
        in_specs=(
            P(both, None), P(both, None), P(both), P(both), P("dp", None), P(both, None), P(both),
        ),
        out_specs=(P(both, None), P(both, None)),
        check_vma=False,
    )
```

```python
import functools

import jax
import jax.numpy as jnp
from jax import lax
from jax.experimental import pallas as pl
from jax.experimental.pallas import tpu as pltpu
from jax.sharding import PartitionSpec as P

MESH = pl.DeviceIdType.MESH
HIGHEST = lax.Precision.HIGHEST
F32 = jnp.float32
BF16 = jnp.bfloat16
LANES = 128
NZ = 8


def dot(a, b, dims=(((1,), (0,)), ((), ())), precision=None):
    return lax.dot_general(a, b, dims, precision=precision, preferred_element_type=F32)


def iota(shape, dim):
    return lax.broadcasted_iota(jnp.int32, shape, dim)


def column(row):
    on = iota((LANES, LANES), 0) == iota((LANES, LANES), 1)
    return jnp.sum(jnp.where(on, row, 0.0), axis=1, keepdims=True)


def kernel(
    cfg, dest_hbm, len_hbm, rate_hbm, batch_hbm, perm_hbm, r_hbm, v_hbm, out_r, out_a,
    dest_ref, slots_ref, len_ref, rate_ref, batch_ref, perm_ref, rbuf, vbuf, send_r, send_a, vals, recv_r, recv_a,
    cols, scales, sums, chooser, member, stats, tsend, trecv, part, st_z, st_y, st_g,
    load_sem, bulk_send, bulk_recv, t_send, t_recv, g_send, g_recv, z_send, z_recv, y_send, y_recv,
):
    n_dp, n_group, piece, span, width = cfg
    rows = n_dp * piece
    n_y = n_dp // NZ
    me = lax.axis_index("dp")
    group = lax.axis_index("group")
    y, z = me // NZ, lax.rem(me, NZ)
    waves = 2 * span // width
    half = waves // 2

    def peer(k):
        return lax.rem(y + k // NZ, n_y) * NZ + lax.rem(z + lax.rem(k, NZ), NZ)

    barrier = pltpu.get_barrier_semaphore()

    def greet(k, c):
        pl.semaphore_signal(barrier, 1, device_id={"dp": peer(k)}, device_id_type=MESH)
        return c

    lax.fori_loop(1, n_dp, greet, 0)

    def greet_group(k, c):
        pl.semaphore_signal(
            barrier, 1, device_id={"group": lax.rem(group + k, n_group)}, device_id_type=MESH
        )
        return c

    lax.fori_loop(1, n_group, greet_group, 0)

    pairs = (
        (dest_hbm, dest_ref), (len_hbm, len_ref), (rate_hbm, rate_ref),
        (batch_hbm, batch_ref), (perm_hbm, perm_ref),
    )
    smalls = [pltpu.make_async_copy(a, b, load_sem.at[i]) for i, (a, b) in enumerate(pairs)]
    quarter = n_dp // 4

    def load(q, i):
        source, target = ((r_hbm, rbuf), (v_hbm, vbuf))[q]
        pieces = pl.ds(i * quarter, quarter)
        return pltpu.make_async_copy(
            source.at[pieces], target.at[pieces], load_sem.at[5 + 4 * q + i]
        )

    for copy in smalls:
        copy.start()
    for i in range(4):
        load(0, i).start()
    for i in range(4):
        load(1, i).start()

    for copy in smalls:
        copy.wait()

    def invert(d, c):
        slot = 0
        for p in range(n_dp):
            slot = jnp.where(dest_ref[0, p] == d, p, slot)
        slots_ref[d] = slot
        return c

    lax.fori_loop(0, n_dp, invert, 0)

    for b in range(2):
        for q, ref in enumerate((len_ref, rate_ref)):
            spread = jnp.broadcast_to(column(ref[b : b + 1, :].astype(F32)), (LANES, LANES))
            per = LANES // piece
            cols[q, per * b : per * (b + 1)] = spread.reshape(per, piece, LANES)

    for i in range(4):
        load(0, i).wait()

    def gather_r(d, c):
        p = slots_ref[d]
        send_r[d] = rbuf[p]
        sums[0, d] = cols[0, p]
        sums[1, d] = cols[1, p]
        return c

    lax.fori_loop(0, n_dp, gather_r, 0)

    pl.semaphore_wait(barrier, n_dp - 1 + n_group - 1)

    def bulk(w, k):
        source, target = (send_r, recv_r) if w < half else (send_a, recv_a)
        lanes = pl.ds((w % half) * width, width)
        return pltpu.make_async_remote_copy(
            source.at[peer(k), :, lanes], target.at[me, :, lanes],
            bulk_send.at[w, k], bulk_recv.at[w, k],
            device_id={"dp": peer(k)}, device_id_type=MESH,
        )

    def start_wave(w):
        def go(k, c):
            bulk(w, k).start()
            return c

        lax.fori_loop(1, n_dp, go, 0)

    start_wave(0)

    for i in range(4):
        load(1, i).wait()

    def gather_v(d, c):
        vals[d] = vbuf[slots_ref[d]]
        return c

    lax.fori_loop(0, n_dp, gather_v, 0)
    recv_r[me] = send_r[me]

    lane = iota((rows, LANES), 1)
    lane_f = lane.astype(F32)
    lengths = sums[0].reshape(rows, LANES).astype(jnp.int32)
    rate = sums[1].reshape(rows, LANES)
    cols[0] = sums[0]
    scales[0] = jnp.exp(-rate)
    scales[1] = jnp.exp(-rate * lane_f)
    scales[2] = jnp.exp(rate * lane_f)
    scales[3] = jnp.exp(-rate * (LANES - lane_f))
    sums[...] = jnp.zeros_like(sums)
    triangle = (iota((LANES, LANES), 0) >= iota((LANES, LANES), 1)).astype(F32)

    def block(i, carry):
        next_head, next_value = carry
        at = span // LANES - 1 - i
        lanes = pl.ds(pl.multiple_of(at * LANES, LANES), LANES)
        position = at * LANES + lane
        length = cols[0].reshape(rows, LANES).astype(jnp.int32)
        reward = send_r[:, :, lanes].astype(F32).reshape(rows, LANES)
        value = vals[:, :, lanes].astype(F32).reshape(rows, LANES)
        valid = position < length
        value_next = jnp.where(lane == LANES - 1, next_value, pltpu.roll(value, LANES - 1, 1))
        value_next = jnp.where(position + 1 < length, value_next, 0.0)
        td = jnp.where(valid, reward + scales[0] * value_next - value, 0.0)
        local = dot(td * scales[1], triangle, precision=HIGHEST) * scales[2]
        total = local + scales[3] * next_head
        rounded = jnp.where(valid, total, 0.0).astype(BF16)
        send_a[:, :, lanes] = rounded.reshape(n_dp, piece, LANES)
        reward = jnp.where(valid, reward, 0.0)
        kept = rounded.astype(F32)
        for q, term in enumerate((reward, kept, reward * reward, kept * kept)):
            sums[q] += term.reshape(n_dp, piece, LANES)
        return total[:, 0:1], value[:, 0:1]

    zero = jnp.zeros((rows, 1), F32)
    lax.fori_loop(0, span // LANES, block, (zero, zero))
    recv_a[me] = send_a[me]

    term_of, row_of = lane // piece, lax.rem(lane, piece)
    own = row_of == lax.rem(iota((rows, LANES), 0), piece)
    packed = jnp.where(own & (term_of == 0), cols[0].reshape(rows, LANES), 0.0)
    for q in range(4):
        total = jnp.sum(sums[q].reshape(rows, LANES), axis=1, keepdims=True)
        packed = jnp.where(own & (term_of == q + 1), total, packed)
    tsend[...] = jnp.sum(packed.reshape(n_dp, piece, LANES), axis=1, keepdims=True)

    for b in range(2):
        here = slice(b * LANES, (b + 1) * LANES)
        order = column(perm_ref[b : b + 1, :].astype(F32)).astype(jnp.int32)
        chooser[b] = (order == iota((LANES, LANES), 1)).astype(BF16)
        batch = column(batch_ref[b : b + 1, :].astype(F32)).astype(jnp.int32)
        member[here] = (batch == iota((LANES, LANES), 1)).astype(F32)

    def terms(k):
        return pltpu.make_async_remote_copy(
            tsend.at[peer(k)], trecv.at[me], t_send.at[k], t_recv.at[k],
            device_id={"dp": peer(k)}, device_id_type=MESH,
        )

    def terms_go(k, c):
        terms(k).start()
        return c

    def terms_wait(k, c):
        terms(k).wait()
        return c

    lax.fori_loop(1, n_dp, terms_go, 0)
    start_wave(1)
    trecv[me] = tsend[me]
    lax.fori_loop(1, n_dp, terms_wait, 0)

    spread = jnp.broadcast_to(trecv[...], (n_dp, piece, LANES)).reshape(rows, LANES)
    spread = jnp.where(own, spread, 0.0)
    select = (iota((LANES, LANES), 0) // piece == iota((LANES, LANES), 1)).astype(F32)
    totals = jnp.zeros((LANES, LANES), F32)
    for b in range(2):
        here = slice(b * LANES, (b + 1) * LANES)
        moved = dot(chooser[b].astype(F32), spread[here], precision=HIGHEST)
        moved = dot(moved, select, precision=HIGHEST)
        stats[4, here] = jnp.broadcast_to(moved[:, 0:1], (LANES, LANES))
        totals += dot(moved, member[here], (((0,), (0,)), ((), ())), precision=HIGHEST)

    def exchange(store, index, sizes, target, send_sem, recv_sem, between):
        store[index] = part[...]

        def copy(k):
            return pltpu.make_async_remote_copy(
                part, store.at[index], send_sem.at[k], recv_sem.at[k],
                device_id=target(k), device_id_type=MESH,
            )

        def go(k, c):
            copy(k).start()
            return c

        def done(k, c):
            copy(k).wait()
            return c

        lax.fori_loop(1, sizes, go, 0)
        between()
        lax.fori_loop(1, sizes, done, 0)
        part[...] = jnp.sum(store[...], axis=0)

    part[...] = totals[0:8]
    exchange(
        st_g, group, n_group, lambda k: {"group": lax.rem(group + k, n_group)},
        g_send, g_recv, lambda: None,
    )
    exchange(
        st_z, z, NZ, lambda k: {"dp": y * NZ + lax.rem(z + k, NZ)},
        z_send, z_recv, lambda: start_wave(2),
    )
    exchange(
        st_y, y, n_y, lambda k: {"dp": lax.rem(y + k, n_y) * NZ + z},
        y_send, y_recv, lambda: start_wave(3),
    )

    total = part[...]
    count = jnp.maximum(total[0:1], 1.0)
    for q in range(2):
        mean = total[1 + q : 2 + q] / count
        spread = total[3 + q : 4 + q] / count - mean * mean
        for s, value in enumerate((mean, lax.rsqrt(spread + 1e-05))):
            picked = jnp.sum(member[...] * value, axis=1, keepdims=True)
            stats[2 * q + s] = jnp.broadcast_to(picked, (rows, LANES))

    tile = 256
    for w in range(waves):
        def wait_wave(k, c):
            bulk(w, k).wait()
            return c

        lax.fori_loop(1, n_dp, wait_wave, 0)
        q = 0 if w < half else 1
        source, out = ((recv_r, out_r), (recv_a, out_a))[q]

        def finish(i, c):
            start = pl.multiple_of((w % half) * width + i * tile, LANES)
            for b in range(2):
                per = LANES // piece
                block = source[per * b : per * (b + 1), :, pl.ds(start, tile)]
                block = block.astype(F32).reshape(LANES, tile).astype(BF16)
                moved = dot(chooser[b], block)
                here = slice(b * LANES, (b + 1) * LANES)
                length = stats[4, here].astype(jnp.int32)
                for s in range(tile // LANES):
                    position = start + s * LANES + iota((LANES, LANES), 1)
                    white = (moved[:, s * LANES : (s + 1) * LANES] - stats[2 * q, here]) * stats[
                        2 * q + 1, here
                    ]
                    out[here, pl.ds(start + s * LANES, LANES)] = jnp.where(
                        position < length, white, 0.0
                    ).astype(BF16)
            return c

        lax.fori_loop(0, width // tile, finish, 0)


def local(rewards, values, lengths, decay_rate, piece_dest, row_perm, minibatch, *, n_dp, n_group):
    rows, span = rewards.shape
    piece = rows // n_dp
    width = span // 2
    vmem = pl.BlockSpec(memory_space=pltpu.VMEM)
    hbm = pl.BlockSpec(memory_space=pltpu.HBM)
    bulk = pltpu.VMEM((n_dp, piece, span), BF16)
    dma = pltpu.SemaphoreType.DMA
    waves = 2 * span // width
    n_y = n_dp // NZ
    return pl.pallas_call(
        functools.partial(kernel, (n_dp, n_group, piece, span, width)),
        out_shape=(jax.ShapeDtypeStruct((rows, span), BF16),) * 2,
        in_specs=[hbm] * 7,
        out_specs=(vmem, vmem),
        scratch_shapes=[
            pltpu.SMEM((1, n_dp), jnp.int32),
            pltpu.SMEM((n_dp,), jnp.int32),
            pltpu.VMEM((2, LANES), jnp.int32),
            pltpu.VMEM((2, LANES), F32),
            pltpu.VMEM((2, LANES), jnp.int32),
            pltpu.VMEM((2, LANES), jnp.int32),
        ]
        + [bulk] * 7
        + [
            pltpu.VMEM((2, n_dp, piece, LANES), F32),
            pltpu.VMEM((4, rows, LANES), F32),
            pltpu.VMEM((4, n_dp, piece, LANES), F32),
            pltpu.VMEM((2, LANES, LANES), BF16),
            pltpu.VMEM((rows, LANES), F32),
            pltpu.VMEM((5, rows, LANES), F32),
            pltpu.VMEM((n_dp, 1, LANES), F32),
            pltpu.VMEM((n_dp, 1, LANES), F32),
            pltpu.VMEM((8, LANES), F32),
            pltpu.VMEM((NZ, 8, LANES), F32),
            pltpu.VMEM((n_y, 8, LANES), F32),
            pltpu.VMEM((n_group, 8, LANES), F32),
            dma((13,)),
            dma((waves, n_dp)), dma((waves, n_dp)),
            dma((n_dp,)), dma((n_dp,)),
            dma((n_group,)), dma((n_group,)),
            dma((NZ,)), dma((NZ,)),
            dma((n_y,)), dma((n_y,)),
        ],
        compiler_params=pltpu.CompilerParams(
            collective_id=0, has_side_effects=True, vmem_limit_bytes=40 * 2**20
        ),
        name="reshuffle",
    )(
        *(
            pltpu.with_memory_space_constraint(array, pltpu.HBM)
            for array in (
                piece_dest,
                lengths.reshape(2, LANES),
                decay_rate.reshape(2, LANES),
                minibatch.reshape(2, LANES),
                row_perm,
                rewards.reshape(n_dp, piece, span),
                values.reshape(n_dp, piece, span),
            )
        )
    )


def solution(mesh):
    both = ("dp", "group")
    return jax.shard_map(
        functools.partial(local, n_dp=mesh.shape["dp"], n_group=mesh.shape["group"]),
        mesh=mesh,
        in_specs=(
            P(both, None), P(both, None), P(both), P(both), P("dp", None), P(both, None), P(both),
        ),
        out_specs=(P(both, None), P(both, None)),
        check_vma=False,
    )
```

```python
import functools

import jax
import jax.numpy as jnp
from jax import lax
from jax.experimental import pallas as pl
from jax.experimental.pallas import tpu as pltpu
from jax.sharding import PartitionSpec as P

MESH = pl.DeviceIdType.MESH
HIGHEST = lax.Precision.HIGHEST
F32 = jnp.float32
BF16 = jnp.bfloat16
LANES = 128
NZ = 8


def dot(a, b, dims=(((1,), (0,)), ((), ())), precision=None):
    return lax.dot_general(a, b, dims, precision=precision, preferred_element_type=F32)


def iota(shape, dim):
    return lax.broadcasted_iota(jnp.int32, shape, dim)


def column(row):
    on = iota((LANES, LANES), 0) == iota((LANES, LANES), 1)
    return jnp.sum(jnp.where(on, row, 0.0), axis=1, keepdims=True)


def whiten(block, chooser, mean, scale, length, start):
    tile = block.shape[-1]
    moved = dot(chooser, block.astype(F32).reshape(LANES, tile).astype(BF16))
    done = []
    for s in range(tile // LANES):
        position = start + s * LANES + iota((LANES, LANES), 1)
        white = (moved[:, s * LANES : (s + 1) * LANES] - mean) * scale
        done.append(jnp.where(position < length, white, 0.0).astype(BF16))
    return jnp.concatenate(done, axis=1)


def kernel(
    cfg, dest_hbm, len_hbm, rate_hbm, batch_hbm, perm_hbm, r_hbm, v_hbm,
    out_r, out_a, last, chooser, stats,
    dest_ref, slots_ref, len_ref, rate_ref, batch_ref, perm_ref, rbuf, vbuf, send_r, send_a, vals, recv_r, recv_a,
    cols, scales, sums, member, stats_r, tsend, trecv, part, st_z, st_y, st_g,
    load_sem, bulk_send, bulk_recv, t_send, t_recv, g_send, g_recv, z_send, z_recv, y_send, y_recv, ready,
):
    n_dp, n_group, piece, span, width = cfg
    rows = n_dp * piece
    n_y = n_dp // NZ
    me = lax.axis_index("dp")
    group = lax.axis_index("group")
    y, z = me // NZ, lax.rem(me, NZ)
    waves = 2 * span // width
    half = waves // 2

    def peer(k):
        return lax.rem(y + k // NZ, n_y) * NZ + lax.rem(z + lax.rem(k, NZ), NZ)

    def near(k):
        return lax.rem(k // 5 + n_y - 1, n_y) * NZ + lax.rem(lax.rem(k, 5) + NZ - 2, NZ)

    def each_near(do):
        def go(k, c):
            do(near(k))
            return c

        lax.fori_loop(0, 7, go, 0)
        lax.fori_loop(8, 15, go, 0)

    def each_far(do):
        def beside(k, c):
            do(lax.rem(k // 3 + n_y - 1, n_y) * NZ + 3 + lax.rem(k, 3))
            return c

        def across(k, c):
            do(2 * NZ + k)
            return c

        lax.fori_loop(0, 9, beside, 0)
        lax.fori_loop(0, NZ, across, 0)

    barrier = pltpu.get_barrier_semaphore()
    each_near(
        lambda k: pl.semaphore_signal(barrier, 1, device_id={"dp": peer(k)}, device_id_type=MESH)
    )

    def greet_group(k, c):
        pl.semaphore_signal(
            barrier, 1, device_id={"group": lax.rem(group + k, n_group)}, device_id_type=MESH
        )
        return c

    lax.fori_loop(1, n_group, greet_group, 0)

    pairs = (
        (dest_hbm, dest_ref), (len_hbm, len_ref), (rate_hbm, rate_ref),
        (batch_hbm, batch_ref), (perm_hbm, perm_ref),
    )
    smalls = [pltpu.make_async_copy(a, b, load_sem.at[i]) for i, (a, b) in enumerate(pairs)]
    quarter = n_dp // 4

    def load(q, i):
        source, target = ((r_hbm, rbuf), (v_hbm, vbuf))[q]
        pieces = pl.ds(i * quarter, quarter)
        return pltpu.make_async_copy(
            source.at[pieces], target.at[pieces], load_sem.at[5 + 4 * q + i]
        )

    for copy in smalls:
        copy.start()
    for i in range(4):
        load(0, i).start()
    for i in range(4):
        load(1, i).start()

    for copy in smalls:
        copy.wait()

    def invert(d, c):
        slot = 0
        for p in range(n_dp):
            slot = jnp.where(dest_ref[0, p] == d, p, slot)
        slots_ref[d] = slot
        return c

    lax.fori_loop(0, n_dp, invert, 0)

    for i in range(4):
        load(0, i).wait()

    def gather_first(d, c):
        send_r[d, :, 0:width] = rbuf[slots_ref[d], :, 0:width]
        return c

    lax.fori_loop(0, n_dp, gather_first, 0)

    pl.semaphore_wait(barrier, 14 + n_group - 1)
    each_near(
        lambda k: pl.semaphore_signal(ready, 1, device_id={"dp": peer(k)}, device_id_type=MESH)
    )

    def bulk(w, k):
        source, target = (send_r, recv_r) if w < half else (send_a, recv_a)
        lanes = pl.ds((w % half) * width, width)
        landing = last.at[me] if w == waves - 1 else target.at[me, :, lanes]
        return pltpu.make_async_remote_copy(
            source.at[peer(k), :, lanes], landing,
            bulk_send.at[w, k], bulk_recv.at[w, k],
            device_id={"dp": peer(k)}, device_id_type=MESH,
        )

    def start_wave(w):
        def go(k, c):
            bulk(w, k).start()
            return c

        lax.fori_loop(1, n_dp, go, 0)

    each_near(lambda k: bulk(0, k).start())

    def gather_rest(d, c):
        send_r[d, :, width:span] = rbuf[slots_ref[d], :, width:span]
        return c

    lax.fori_loop(0, n_dp, gather_rest, 0)

    pl.semaphore_wait(ready, 14)
    each_far(lambda k: bulk(0, k).start())

    for b in range(2):
        for q, ref in enumerate((len_ref, rate_ref)):
            spread = jnp.broadcast_to(column(ref[b : b + 1, :].astype(F32)), (LANES, LANES))
            per = LANES // piece
            cols[q, per * b : per * (b + 1)] = spread.reshape(per, piece, LANES)

    for i in range(4):
        load(1, i).wait()

    def gather_v(d, c):
        p = slots_ref[d]
        vals[d] = vbuf[p]
        sums[0, d] = cols[0, p]
        sums[1, d] = cols[1, p]
        return c

    lax.fori_loop(0, n_dp, gather_v, 0)
    recv_r[me] = send_r[me]

    lane = iota((rows, LANES), 1)
    lane_f = lane.astype(F32)
    lengths = sums[0].reshape(rows, LANES).astype(jnp.int32)
    rate = sums[1].reshape(rows, LANES)
    cols[0] = sums[0]
    scales[0] = jnp.exp(-rate)
    scales[1] = jnp.exp(-rate * lane_f)
    scales[2] = jnp.exp(rate * lane_f)
    scales[3] = jnp.exp(-rate * (LANES - lane_f))
    sums[...] = jnp.zeros_like(sums)
    triangle = (iota((LANES, LANES), 0) >= iota((LANES, LANES), 1)).astype(F32)

    def block(i, carry):
        next_head, next_value = carry
        at = span // LANES - 1 - i
        lanes = pl.ds(pl.multiple_of(at * LANES, LANES), LANES)
        position = at * LANES + lane
        length = cols[0].reshape(rows, LANES).astype(jnp.int32)
        reward = send_r[:, :, lanes].astype(F32).reshape(rows, LANES)
        value = vals[:, :, lanes].astype(F32).reshape(rows, LANES)
        valid = position < length
        value_next = jnp.where(lane == LANES - 1, next_value, pltpu.roll(value, LANES - 1, 1))
        value_next = jnp.where(position + 1 < length, value_next, 0.0)
        td = jnp.where(valid, reward + scales[0] * value_next - value, 0.0)
        local = dot(td * scales[1], triangle, precision=HIGHEST) * scales[2]
        total = local + scales[3] * next_head
        rounded = jnp.where(valid, total, 0.0).astype(BF16)
        send_a[:, :, lanes] = rounded.reshape(n_dp, piece, LANES)
        reward = jnp.where(valid, reward, 0.0)
        kept = rounded.astype(F32)
        for q, term in enumerate((reward, kept, reward * reward, kept * kept)):
            sums[q] += term.reshape(n_dp, piece, LANES)
        return total[:, 0:1], value[:, 0:1]

    zero = jnp.zeros((rows, 1), F32)
    lax.fori_loop(0, span // LANES, block, (zero, zero))
    recv_a[me] = send_a[me, :, 0 : span - width]
    last[me] = send_a[me, :, span - width : span]

    term_of, row_of = lane // piece, lax.rem(lane, piece)
    own = row_of == lax.rem(iota((rows, LANES), 0), piece)
    packed = jnp.where(own & (term_of == 0), cols[0].reshape(rows, LANES), 0.0)
    for q in range(4):
        total = jnp.sum(sums[q].reshape(rows, LANES), axis=1, keepdims=True)
        packed = jnp.where(own & (term_of == q + 1), total, packed)
    tsend[...] = jnp.sum(packed.reshape(n_dp, piece, LANES), axis=1, keepdims=True)

    for b in range(2):
        here = slice(b * LANES, (b + 1) * LANES)
        order = column(perm_ref[b : b + 1, :].astype(F32)).astype(jnp.int32)
        chooser[b] = (order == iota((LANES, LANES), 1)).astype(BF16)
        batch = column(batch_ref[b : b + 1, :].astype(F32)).astype(jnp.int32)
        member[here] = (batch == iota((LANES, LANES), 1)).astype(F32)

    def terms(k):
        return pltpu.make_async_remote_copy(
            tsend.at[peer(k)], trecv.at[me], t_send.at[k], t_recv.at[k],
            device_id={"dp": peer(k)}, device_id_type=MESH,
        )

    def terms_go(k, c):
        terms(k).start()
        return c

    def terms_wait(k, c):
        terms(k).wait()
        return c

    lax.fori_loop(1, n_dp, terms_go, 0)
    start_wave(1)
    trecv[me] = tsend[me]
    lax.fori_loop(1, n_dp, terms_wait, 0)

    spread = jnp.broadcast_to(trecv[...], (n_dp, piece, LANES)).reshape(rows, LANES)
    spread = jnp.where(own, spread, 0.0)
    select = (iota((LANES, LANES), 0) // piece == iota((LANES, LANES), 1)).astype(F32)
    totals = jnp.zeros((LANES, LANES), F32)
    for b in range(2):
        here = slice(b * LANES, (b + 1) * LANES)
        moved = dot(chooser[b].astype(F32), spread[here], precision=HIGHEST)
        moved = dot(moved, select, precision=HIGHEST)
        stats[2, here] = jnp.broadcast_to(moved[:, 0:1], (LANES, LANES))
        totals += dot(moved, member[here], (((0,), (0,)), ((), ())), precision=HIGHEST)

    def exchange(store, index, sizes, target, send_sem, recv_sem, between):
        store[index] = part[...]

        def copy(k):
            return pltpu.make_async_remote_copy(
                part, store.at[index], send_sem.at[k], recv_sem.at[k],
                device_id=target(k), device_id_type=MESH,
            )

        def go(k, c):
            copy(k).start()
            return c

        def done(k, c):
            copy(k).wait()
            return c

        lax.fori_loop(1, sizes, go, 0)
        between()
        lax.fori_loop(1, sizes, done, 0)
        part[...] = jnp.sum(store[...], axis=0)

    part[...] = totals[0:8]
    exchange(
        st_g, group, n_group, lambda k: {"group": lax.rem(group + k, n_group)},
        g_send, g_recv, lambda: None,
    )
    exchange(
        st_z, z, NZ, lambda k: {"dp": y * NZ + lax.rem(z + k, NZ)},
        z_send, z_recv, lambda: start_wave(2),
    )
    exchange(
        st_y, y, n_y, lambda k: {"dp": lax.rem(y + k, n_y) * NZ + z},
        y_send, y_recv, lambda: start_wave(3),
    )

    total = part[...]
    count = jnp.maximum(total[0:1], 1.0)
    for q in range(2):
        mean = total[1 + q : 2 + q] / count
        spread = total[3 + q : 4 + q] / count - mean * mean
        for s, value in enumerate((mean, lax.rsqrt(spread + 1e-05))):
            picked = jnp.sum(member[...] * value, axis=1, keepdims=True)
            (stats_r, stats)[q][s] = jnp.broadcast_to(picked, (rows, LANES))

    tile = 256
    for w in range(waves):
        def wait_wave(k, c):
            bulk(w, k).wait()
            return c

        lax.fori_loop(1, n_dp, wait_wave, 0)
        if w == waves - 1:
            break
        source, out, moments = ((recv_r, out_r, stats_r), (recv_a, out_a, stats))[w // half]

        def finish(i, c):
            start = pl.multiple_of((w % half) * width + i * tile, LANES)
            for b in range(2):
                per = LANES // piece
                here = slice(b * LANES, (b + 1) * LANES)
                out[here, pl.ds(start, tile)] = whiten(
                    source[per * b : per * (b + 1), :, pl.ds(start, tile)], chooser[b],
                    moments[0, here], moments[1, here], stats[2, here].astype(jnp.int32), start,
                )
            return c

        lax.fori_loop(0, width // tile, finish, 0)


def finish_kernel(cfg, white_r, white_a, last, chooser, stats, out_r, out_a, white, sem):
    piece, span, width = cfg
    rows = white_r.shape[0]
    ready = span - width
    copies = []

    def send(source, target):
        copy = pltpu.make_async_copy(source, target, sem.at[len(copies)])
        copy.start()
        copies.append(copy)

    for i in range(4):
        here = pl.ds(i * (rows // 4), rows // 4)
        send(white_r.at[here], out_r.at[here])
        send(white_a.at[here], out_a.at[here, 0:ready])
    tile = 512
    for i in range(width // tile):
        lanes = slice(i * tile, (i + 1) * tile)
        for b in range(2):
            per = LANES // piece
            here = slice(b * LANES, (b + 1) * LANES)
            white[here, lanes] = whiten(
                last[per * b : per * (b + 1), :, lanes], chooser[b],
                stats[0, here], stats[1, here], stats[2, here].astype(jnp.int32), ready + i * tile,
            )
        send(white.at[:, lanes], out_a.at[:, ready + i * tile : ready + (i + 1) * tile])
    for copy in copies:
        copy.wait()


def local(rewards, values, lengths, decay_rate, piece_dest, row_perm, minibatch, *, n_dp, n_group):
    rows, span = rewards.shape
    piece = rows // n_dp
    width = span // 2
    vmem = pl.BlockSpec(memory_space=pltpu.VMEM)
    hbm = pl.BlockSpec(memory_space=pltpu.HBM)
    bulk = pltpu.VMEM((n_dp, piece, span), BF16)
    dma = pltpu.SemaphoreType.DMA
    waves = 2 * span // width
    n_y = n_dp // NZ
    result = jax.ShapeDtypeStruct((rows, span), BF16)
    parts = pl.pallas_call(
        functools.partial(kernel, (n_dp, n_group, piece, span, width)),
        out_shape=(
            result,
            jax.ShapeDtypeStruct((rows, span - width), BF16),
            jax.ShapeDtypeStruct((n_dp, piece, width), BF16),
            jax.ShapeDtypeStruct((2, LANES, LANES), BF16),
            jax.ShapeDtypeStruct((3, rows, LANES), F32),
        ),
        in_specs=[hbm] * 7,
        out_specs=(vmem,) * 5,
        scratch_shapes=[
            pltpu.SMEM((1, n_dp), jnp.int32),
            pltpu.SMEM((n_dp,), jnp.int32),
            pltpu.VMEM((2, LANES), jnp.int32),
            pltpu.VMEM((2, LANES), F32),
            pltpu.VMEM((2, LANES), jnp.int32),
            pltpu.VMEM((2, LANES), jnp.int32),
        ]
        + [bulk] * 6
        + [
            pltpu.VMEM((n_dp, piece, span - width), BF16),
            pltpu.VMEM((2, n_dp, piece, LANES), F32),
            pltpu.VMEM((4, rows, LANES), F32),
            pltpu.VMEM((4, n_dp, piece, LANES), F32),
            pltpu.VMEM((rows, LANES), F32),
            pltpu.VMEM((2, rows, LANES), F32),
            pltpu.VMEM((n_dp, 1, LANES), F32),
            pltpu.VMEM((n_dp, 1, LANES), F32),
            pltpu.VMEM((8, LANES), F32),
            pltpu.VMEM((NZ, 8, LANES), F32),
            pltpu.VMEM((n_y, 8, LANES), F32),
            pltpu.VMEM((n_group, 8, LANES), F32),
            dma((13,)),
            dma((waves, n_dp)), dma((waves, n_dp)),
            dma((n_dp,)), dma((n_dp,)),
            dma((n_group,)), dma((n_group,)),
            dma((NZ,)), dma((NZ,)),
            dma((n_y,)), dma((n_y,)),
            pltpu.SemaphoreType.REGULAR,
        ],
        compiler_params=pltpu.CompilerParams(
            collective_id=0, has_side_effects=True, vmem_limit_bytes=40 * 2**20
        ),
        name="reshuffle",
    )(
        *(
            pltpu.with_memory_space_constraint(array, pltpu.HBM)
            for array in (
                piece_dest,
                lengths.reshape(2, LANES),
                decay_rate.reshape(2, LANES),
                minibatch.reshape(2, LANES),
                row_perm,
                rewards.reshape(n_dp, piece, span),
                values.reshape(n_dp, piece, span),
            )
        )
    )
    return pl.pallas_call(
        functools.partial(finish_kernel, (piece, span, width)),
        out_shape=(result, result),
        in_specs=[vmem] * 5,
        out_specs=(hbm, hbm),
        scratch_shapes=[pltpu.VMEM((rows, width), BF16), dma((12,))],
        compiler_params=pltpu.CompilerParams(vmem_limit_bytes=16 * 2**20),
        name="finish",
    )(*parts)


def solution(mesh):
    both = ("dp", "group")
    return jax.shard_map(
        functools.partial(local, n_dp=mesh.shape["dp"], n_group=mesh.shape["group"]),
        mesh=mesh,
        in_specs=(
            P(both, None), P(both, None), P(both), P(both), P("dp", None), P(both, None), P(both),
        ),
        out_specs=(P(both, None), P(both, None)),
        check_vma=False,
    )
```

```python
import functools

import jax
import jax.numpy as jnp
from jax import lax
from jax.experimental import pallas as pl
from jax.experimental.pallas import tpu as pltpu
from jax.sharding import PartitionSpec as P

MESH = pl.DeviceIdType.MESH
HIGHEST = lax.Precision.HIGHEST
F32 = jnp.float32
BF16 = jnp.bfloat16
LANES = 128
NZ = 8
CHUNKS = ((0, 0, 1), (0, 1, 1), (0, 2, 2), (1, 0, 2), (1, 2, 2))
STRAIGHT = ((0, 0, 4), (1, 0, 2), (1, 2, 2))
STEPS = (4, 3, 5, 2, 6, 1, 7)


def dot(a, b, dims=(((1,), (0,)), ((), ())), precision=None):
    return lax.dot_general(a, b, dims, precision=precision, preferred_element_type=F32)


def iota(shape, dim):
    return lax.broadcasted_iota(jnp.int32, shape, dim)


def column(row):
    on = iota((LANES, LANES), 0) == iota((LANES, LANES), 1)
    return jnp.sum(jnp.where(on, row, 0.0), axis=1, keepdims=True)


def whiten(source, y, b, lanes, chooser, mean, scale, length, start):
    n_y = source.shape[0]
    half = n_y // 2
    pieces = [source[lax.rem(y - b * half - h + n_y, n_y), :, :, lanes] for h in range(half)]
    block = jnp.concatenate([p.astype(F32) for p in pieces], axis=0)
    tile = block.shape[-1]
    moved = dot(chooser, block.reshape(LANES, tile).astype(BF16))
    done = []
    for s in range(tile // LANES):
        position = start + s * LANES + iota((LANES, LANES), 1)
        white = (moved[:, s * LANES : (s + 1) * LANES] - mean) * scale
        done.append(jnp.where(position < length, white, 0.0).astype(BF16))
    return jnp.concatenate(done, axis=1)


def kernel(
    cfg, dest_hbm, len_hbm, rate_hbm, batch_hbm, perm_hbm, r_hbm, v_hbm,
    out_r, out_a, last, chooser, stats,
    dest_ref, slots_ref, len_ref, rate_ref, batch_ref, perm_ref, rbuf, vbuf, send_r, send_a, vals, recv_r, recv_a,
    relay_0, relay_1, relay_2, relay_3, relay_4,
    cols, scales, sums, member, stats_r, tsend, trelay, trecv, part, st_z, st_y, st_g,
    load_sem, y_leg_send, y_leg_recv, z_leg_send, z_leg_recv, a_send, a_recv,
    t1_send, t1_recv, t2_send, t2_recv, g_send, g_recv, z_send, z_recv, y_send, y_recv,
):
    n_dp, n_group, piece, span = cfg
    rows = n_dp * piece
    n_y = n_dp // NZ
    unit = span // 4
    relays = (relay_0, relay_1, relay_2, relay_3, relay_4)
    final = len(CHUNKS) - 1
    me = lax.axis_index("dp")
    group = lax.axis_index("group")
    y, z = me // NZ, lax.rem(me, NZ)

    def along_y(j):
        return lax.rem(y + j, n_y)

    def along_z(k):
        return lax.rem(z + k, NZ)

    def remote(source, target, send_sem, recv_sem, place):
        return pltpu.make_async_remote_copy(
            source, target, send_sem, recv_sem, device_id=place, device_id_type=MESH
        )

    barrier = pltpu.get_barrier_semaphore()
    for j in range(1, n_y):
        pl.semaphore_signal(
            barrier, 1, device_id={"dp": along_y(j) * NZ + z}, device_id_type=MESH
        )
    for k in range(1, NZ):
        pl.semaphore_signal(
            barrier, 1, device_id={"dp": y * NZ + along_z(k)}, device_id_type=MESH
        )

    def greet_group(k, c):
        pl.semaphore_signal(
            barrier, 1, device_id={"group": lax.rem(group + k, n_group)}, device_id_type=MESH
        )
        return c

    lax.fori_loop(1, n_group, greet_group, 0)

    pairs = (
        (dest_hbm, dest_ref), (len_hbm, len_ref), (rate_hbm, rate_ref),
        (batch_hbm, batch_ref), (perm_hbm, perm_ref),
    )
    smalls = [pltpu.make_async_copy(a, b, load_sem.at[i]) for i, (a, b) in enumerate(pairs)]
    quarter = n_dp // 4

    def load(q, i):
        source, target = ((r_hbm, rbuf), (v_hbm, vbuf))[q]
        pieces = pl.ds(i * quarter, quarter)
        return pltpu.make_async_copy(
            source.at[pieces], target.at[pieces], load_sem.at[5 + 4 * q + i]
        )

    for copy in smalls:
        copy.start()
    for i in range(4):
        load(0, i).start()
    for i in range(4):
        load(1, i).start()

    for copy in smalls:
        copy.wait()

    def invert(d, c):
        slot = 0
        for p in range(n_dp):
            slot = jnp.where(dest_ref[0, p] == d, p, slot)
        slots_ref[d] = slot
        return c

    lax.fori_loop(0, n_dp, invert, 0)

    for i in range(4):
        load(0, i).wait()

    def gather_r(d, c):
        send_r[d] = rbuf[slots_ref[d]]
        return c

    lax.fori_loop(0, n_dp, gather_r, 0)

    pl.semaphore_wait(barrier, n_y - 1 + NZ - 1 + n_group - 1)

    def y_leg(w, j):
        q, first, width = CHUNKS[w]
        source = (send_r, send_a)[q].at[pl.ds(along_y(j) * NZ, NZ), :, pl.ds(first * unit, width * unit)]
        return remote(
            source, relays[w].at[j - 1], y_leg_send.at[w, j], y_leg_recv.at[w, j],
            {"dp": along_y(j) * NZ + z},
        )

    def z_leg(w, k):
        q, first, width = CHUNKS[w]
        lanes = pl.ds(first * unit, width * unit)
        others = pl.ds(1, n_y - 1)
        target = last.at[others, z] if w == final else (recv_r, recv_a)[q].at[others, z, :, lanes]
        return remote(
            relays[w].at[:, along_z(k)], target, z_leg_send.at[w, k], z_leg_recv.at[w, k],
            {"dp": y * NZ + along_z(k)},
        )

    def straight(p, k):
        q, first, width = STRAIGHT[p]
        source = (send_r, send_a)[q].at[y * NZ + along_z(k), :, pl.ds(first * unit, width * unit)]
        return remote(
            source, (recv_r, recv_a, last)[p].at[0, z], a_send.at[p, k], a_recv.at[p, k],
            {"dp": y * NZ + along_z(k)},
        )

    def start_y_leg(w):
        for j in range(1, n_y):
            y_leg(w, j).start()

    def start_straight(p):
        for k in STEPS:
            straight(p, k).start()

    def forward(w):
        for j in range(1, n_y):
            y_leg(w, j).wait_recv()
        for k in STEPS:
            z_leg(w, k).start()
        q, first, width = CHUNKS[w]
        for j in range(1, n_y):
            if w == final:
                last[j, z] = relays[w][j - 1, z]
            else:
                (recv_r, recv_a)[q][j, z, :, first * unit : (first + width) * unit] = relays[w][j - 1, z]

    start_y_leg(0)
    start_straight(0)
    start_y_leg(1)
    start_y_leg(2)

    for b in range(2):
        for q, ref in enumerate((len_ref, rate_ref)):
            spread = jnp.broadcast_to(column(ref[b : b + 1, :].astype(F32)), (LANES, LANES))
            per = LANES // piece
            cols[q, per * b : per * (b + 1)] = spread.reshape(per, piece, LANES)

    for i in range(4):
        load(1, i).wait()

    def gather_v(d, c):
        p = slots_ref[d]
        vals[d] = vbuf[p]
        sums[0, d] = cols[0, p]
        sums[1, d] = cols[1, p]
        return c

    lax.fori_loop(0, n_dp, gather_v, 0)
    recv_r[0, z] = send_r[me]

    lane = iota((rows, LANES), 1)
    lane_f = lane.astype(F32)
    lengths = sums[0].reshape(rows, LANES).astype(jnp.int32)
    rate = sums[1].reshape(rows, LANES)
    cols[0] = sums[0]
    scales[0] = jnp.exp(-rate)
    scales[1] = jnp.exp(-rate * lane_f)
    scales[2] = jnp.exp(rate * lane_f)
    scales[3] = jnp.exp(-rate * (LANES - lane_f))
    sums[...] = jnp.zeros_like(sums)
    triangle = (iota((LANES, LANES), 0) >= iota((LANES, LANES), 1)).astype(F32)

    def block(i, carry):
        next_head, next_value = carry
        at = span // LANES - 1 - i
        lanes = pl.ds(pl.multiple_of(at * LANES, LANES), LANES)
        position = at * LANES + lane
        length = cols[0].reshape(rows, LANES).astype(jnp.int32)
        reward = send_r[:, :, lanes].astype(F32).reshape(rows, LANES)
        value = vals[:, :, lanes].astype(F32).reshape(rows, LANES)
        valid = position < length
        value_next = jnp.where(lane == LANES - 1, next_value, pltpu.roll(value, LANES - 1, 1))
        value_next = jnp.where(position + 1 < length, value_next, 0.0)
        td = jnp.where(valid, reward + scales[0] * value_next - value, 0.0)
        local = dot(td * scales[1], triangle, precision=HIGHEST) * scales[2]
        total = local + scales[3] * next_head
        rounded = jnp.where(valid, total, 0.0).astype(BF16)
        send_a[:, :, lanes] = rounded.reshape(n_dp, piece, LANES)
        reward = jnp.where(valid, reward, 0.0)
        kept = rounded.astype(F32)
        for q, term in enumerate((reward, kept, reward * reward, kept * kept)):
            sums[q] += term.reshape(n_dp, piece, LANES)
        return total[:, 0:1], value[:, 0:1]

    zero = jnp.zeros((rows, 1), F32)
    third = span // LANES // 3
    carry = lax.fori_loop(0, third, block, (zero, zero))
    forward(0)
    carry = lax.fori_loop(third, 2 * third, block, carry)
    forward(1)
    lax.fori_loop(2 * third, span // LANES, block, carry)
    recv_a[0, z] = send_a[me, :, 0 : span // 2]
    last[0, z] = send_a[me, :, span // 2 : span]

    term_of, row_of = lane // piece, lax.rem(lane, piece)
    own = row_of == lax.rem(iota((rows, LANES), 0), piece)
    packed = jnp.where(own & (term_of == 0), cols[0].reshape(rows, LANES), 0.0)
    for q in range(4):
        total = jnp.sum(sums[q].reshape(rows, LANES), axis=1, keepdims=True)
        packed = jnp.where(own & (term_of == q + 1), total, packed)
    tsend[...] = jnp.sum(packed.reshape(n_dp, piece, LANES), axis=1, keepdims=True)

    for b in range(2):
        here = slice(b * LANES, (b + 1) * LANES)
        order = column(perm_ref[b : b + 1, :].astype(F32)).astype(jnp.int32)
        chooser[b] = (order == iota((LANES, LANES), 1)).astype(BF16)
        batch = column(batch_ref[b : b + 1, :].astype(F32)).astype(jnp.int32)
        member[here] = (batch == iota((LANES, LANES), 1)).astype(F32)

    def terms_y(j):
        return remote(
            tsend.at[pl.ds(along_y(j) * NZ, NZ)], trelay.at[j], t1_send.at[j], t1_recv.at[j],
            {"dp": along_y(j) * NZ + z},
        )

    def terms_z(k):
        return remote(
            trelay.at[:, along_z(k)], trecv.at[:, z], t2_send.at[k], t2_recv.at[k],
            {"dp": y * NZ + along_z(k)},
        )

    trelay[0] = tsend[pl.ds(y * NZ, NZ)]
    for j in range(1, n_y):
        terms_y(j).start()
    start_y_leg(3)
    start_y_leg(4)
    for j in range(1, n_y):
        terms_y(j).wait()
    for k in STEPS:
        terms_z(k).start()
    forward(2)
    trecv[:, z] = trelay[:, z]
    for k in STEPS:
        terms_z(k).wait()

    ordered = [trecv[lax.rem(y - h + n_y, n_y)] for h in range(n_y)]
    spread = jnp.concatenate(ordered, axis=0)
    spread = jnp.broadcast_to(spread, (n_dp, piece, LANES)).reshape(rows, LANES)
    spread = jnp.where(own, spread, 0.0)
    select = (iota((LANES, LANES), 0) // piece == iota((LANES, LANES), 1)).astype(F32)
    totals = jnp.zeros((LANES, LANES), F32)
    for b in range(2):
        here = slice(b * LANES, (b + 1) * LANES)
        moved = dot(chooser[b].astype(F32), spread[here], precision=HIGHEST)
        moved = dot(moved, select, precision=HIGHEST)
        stats[2, here] = jnp.broadcast_to(moved[:, 0:1], (LANES, LANES))
        totals += dot(moved, member[here], (((0,), (0,)), ((), ())), precision=HIGHEST)

    def exchange(store, index, sizes, target, send_sem, recv_sem, between):
        store[index] = part[...]

        def copy(k):
            return pltpu.make_async_remote_copy(
                part, store.at[index], send_sem.at[k], recv_sem.at[k],
                device_id=target(k), device_id_type=MESH,
            )

        def go(k, c):
            copy(k).start()
            return c

        def done(k, c):
            copy(k).wait()
            return c

        lax.fori_loop(1, sizes, go, 0)
        between()
        lax.fori_loop(1, sizes, done, 0)
        part[...] = jnp.sum(store[...], axis=0)

    part[...] = totals[0:8]
    exchange(
        st_g, group, n_group, lambda k: {"group": lax.rem(group + k, n_group)},
        g_send, g_recv, lambda: None,
    )
    def advantage_straight():
        start_straight(1)
        start_straight(2)

    exchange(
        st_z, z, NZ, lambda k: {"dp": y * NZ + along_z(k)}, z_send, z_recv, advantage_straight
    )
    exchange(
        st_y, y, n_y, lambda k: {"dp": along_y(k) * NZ + z}, y_send, y_recv, lambda: forward(3)
    )
    forward(final)

    total = part[...]
    count = jnp.maximum(total[0:1], 1.0)
    for q in range(2):
        mean = total[1 + q : 2 + q] / count
        spread = total[3 + q : 4 + q] / count - mean * mean
        for s, value in enumerate((mean, lax.rsqrt(spread + 1e-05))):
            picked = jnp.sum(member[...] * value, axis=1, keepdims=True)
            (stats_r, stats)[q][s] = jnp.broadcast_to(picked, (rows, LANES))

    tile = 256
    for w, (q, first, width) in enumerate(CHUNKS):
        for p, (kind, begin, _) in enumerate(STRAIGHT):
            if (kind, begin) == (q, first):
                for k in STEPS:
                    straight(p, k).wait()
        for k in STEPS:
            z_leg(w, k).wait()
        if w == final:
            break
        source, out, moments = ((recv_r, out_r, stats_r), (recv_a, out_a, stats))[q]

        def finish(i, c):
            start = pl.multiple_of(first * unit + i * tile, LANES)
            for b in range(2):
                here = slice(b * LANES, (b + 1) * LANES)
                out[here, pl.ds(start, tile)] = whiten(
                    source, y, b, pl.ds(start, tile), chooser[b],
                    moments[0, here], moments[1, here], stats[2, here].astype(jnp.int32), start,
                )
            return c

        lax.fori_loop(0, width * unit // tile, finish, 0)
    for w in range(len(CHUNKS)):
        for j in range(1, n_y):
            y_leg(w, j).wait_send()


def finish_kernel(n_dp, white_r, white_a, last, chooser, stats, out_r, out_a, white, sem):
    rows, width = white.shape
    ready = white_a.shape[1]
    y = lax.axis_index("dp") // NZ
    copies = []

    def send(source, target):
        copy = pltpu.make_async_copy(source, target, sem.at[len(copies)])
        copy.start()
        copies.append(copy)

    for i in range(4):
        here = pl.ds(i * (rows // 4), rows // 4)
        send(white_r.at[here], out_r.at[here])
        send(white_a.at[here], out_a.at[here, 0:ready])
    tile = 512
    for i in range(width // tile):
        lanes = slice(i * tile, (i + 1) * tile)
        for b in range(2):
            here = slice(b * LANES, (b + 1) * LANES)
            white[here, lanes] = whiten(
                last, y, b, lanes, chooser[b],
                stats[0, here], stats[1, here], stats[2, here].astype(jnp.int32), ready + i * tile,
            )
        send(white.at[:, lanes], out_a.at[:, ready + i * tile : ready + (i + 1) * tile])
    for copy in copies:
        copy.wait()


def local(rewards, values, lengths, decay_rate, piece_dest, row_perm, minibatch, *, n_dp, n_group):
    rows, span = rewards.shape
    piece = rows // n_dp
    half = span // 2
    unit = span // 4
    n_y = n_dp // NZ
    vmem = pl.BlockSpec(memory_space=pltpu.VMEM)
    hbm = pl.BlockSpec(memory_space=pltpu.HBM)
    bulk = pltpu.VMEM((n_dp, piece, span), BF16)
    dma = pltpu.SemaphoreType.DMA
    chunks = len(CHUNKS)
    result = jax.ShapeDtypeStruct((rows, span), BF16)
    parts = pl.pallas_call(
        functools.partial(kernel, (n_dp, n_group, piece, span)),
        out_shape=(
            result,
            jax.ShapeDtypeStruct((rows, half), BF16),
            jax.ShapeDtypeStruct((n_y, NZ, piece, half), BF16),
            jax.ShapeDtypeStruct((2, LANES, LANES), BF16),
            jax.ShapeDtypeStruct((3, rows, LANES), F32),
        ),
        in_specs=[hbm] * 7,
        out_specs=(vmem,) * 5,
        scratch_shapes=[
            pltpu.SMEM((1, n_dp), jnp.int32),
            pltpu.SMEM((n_dp,), jnp.int32),
            pltpu.VMEM((2, LANES), jnp.int32),
            pltpu.VMEM((2, LANES), F32),
            pltpu.VMEM((2, LANES), jnp.int32),
            pltpu.VMEM((2, LANES), jnp.int32),
        ]
        + [bulk] * 5
        + [
            pltpu.VMEM((n_y, NZ, piece, span), BF16),
            pltpu.VMEM((n_y, NZ, piece, half), BF16),
        ]
        + [pltpu.VMEM((n_y - 1, NZ, piece, w * unit), BF16) for _, _, w in CHUNKS]
        + [
            pltpu.VMEM((2, n_dp, piece, LANES), F32),
            pltpu.VMEM((4, rows, LANES), F32),
            pltpu.VMEM((4, n_dp, piece, LANES), F32),
            pltpu.VMEM((rows, LANES), F32),
            pltpu.VMEM((2, rows, LANES), F32),
            pltpu.VMEM((n_dp, 1, LANES), F32),
            pltpu.VMEM((n_y, NZ, 1, LANES), F32),
            pltpu.VMEM((n_y, NZ, 1, LANES), F32),
            pltpu.VMEM((8, LANES), F32),
            pltpu.VMEM((NZ, 8, LANES), F32),
            pltpu.VMEM((n_y, 8, LANES), F32),
            pltpu.VMEM((n_group, 8, LANES), F32),
            dma((13,)),
            dma((chunks, n_y)), dma((chunks, n_y)),
            dma((chunks, NZ)), dma((chunks, NZ)),
            dma((len(STRAIGHT), NZ)), dma((len(STRAIGHT), NZ)),
            dma((n_y,)), dma((n_y,)),
            dma((NZ,)), dma((NZ,)),
            dma((n_group,)), dma((n_group,)),
            dma((NZ,)), dma((NZ,)),
            dma((n_y,)), dma((n_y,)),
        ],
        compiler_params=pltpu.CompilerParams(
            collective_id=0, has_side_effects=True, vmem_limit_bytes=40 * 2**20
        ),
        name="reshuffle",
    )(
        *(
            pltpu.with_memory_space_constraint(array, pltpu.HBM)
            for array in (
                piece_dest,
                lengths.reshape(2, LANES),
                decay_rate.reshape(2, LANES),
                minibatch.reshape(2, LANES),
                row_perm,
                rewards.reshape(n_dp, piece, span),
                values.reshape(n_dp, piece, span),
            )
        )
    )
    return pl.pallas_call(
        functools.partial(finish_kernel, n_dp),
        out_shape=(result, result),
        in_specs=[vmem] * 5,
        out_specs=(hbm, hbm),
        scratch_shapes=[pltpu.VMEM((rows, half), BF16), dma((12,))],
        compiler_params=pltpu.CompilerParams(vmem_limit_bytes=16 * 2**20),
        name="finish",
    )(*parts)


def solution(mesh):
    both = ("dp", "group")
    return jax.shard_map(
        functools.partial(local, n_dp=mesh.shape["dp"], n_group=mesh.shape["group"]),
        mesh=mesh,
        in_specs=(
            P(both, None), P(both, None), P(both), P(both), P("dp", None), P(both, None), P(both),
        ),
        out_specs=(P(both, None), P(both, None)),
        check_vma=False,
    )
```

```python
import functools

import jax
import jax.numpy as jnp
from jax import lax
from jax.experimental import pallas as pl
from jax.experimental.pallas import tpu as pltpu
from jax.sharding import PartitionSpec as P

MESH = pl.DeviceIdType.MESH
HIGHEST = lax.Precision.HIGHEST
F32 = jnp.float32
BF16 = jnp.bfloat16
LANES = 128
NZ = 8
CHUNKS = ((0, 0, 1), (0, 1, 1), (0, 2, 2), (1, 0, 2), (1, 2, 2))
STRAIGHT = ((0, 0, 4), (1, 0, 2), (1, 2, 2))
STEPS = (4, 3, 5, 2, 6, 1, 7)
PLANES = (0, 1, 2, 3, 7, 4, 6, 5)


def dot(a, b, dims=(((1,), (0,)), ((), ())), precision=None):
    return lax.dot_general(a, b, dims, precision=precision, preferred_element_type=F32)


def iota(shape, dim):
    return lax.broadcasted_iota(jnp.int32, shape, dim)


def column(row):
    on = iota((LANES, LANES), 0) == iota((LANES, LANES), 1)
    return jnp.sum(jnp.where(on, row, 0.0), axis=1, keepdims=True)


def whiten(source, y, b, lanes, chooser, mean, scale, length, start):
    n_y = source.shape[0]
    half = n_y // 2
    pieces = [source[lax.rem(y - b * half - h + n_y, n_y), :, :, lanes] for h in range(half)]
    block = jnp.concatenate([p.astype(F32) for p in pieces], axis=0)
    tile = block.shape[-1]
    moved = dot(chooser, block.reshape(LANES, tile).astype(BF16))
    done = []
    for s in range(tile // LANES):
        position = start + s * LANES + iota((LANES, LANES), 1)
        white = (moved[:, s * LANES : (s + 1) * LANES] - mean) * scale
        done.append(jnp.where(position < length, white, 0.0).astype(BF16))
    return jnp.concatenate(done, axis=1)


def kernel(
    cfg, dest_hbm, len_hbm, rate_hbm, batch_hbm, perm_hbm, r_hbm, v_hbm,
    out_r, out_a, last, chooser, stats,
    dest_ref, slots_ref, len_ref, rate_ref, batch_ref, perm_ref, rbuf, vbuf, send_r, send_a, vals, recv_r, recv_a,
    relay_0, relay_1, relay_2, relay_3, relay_4,
    cols, scales, sums, member, stats_r, tsend, trelay, trecv, part, st_z, st_y, st_g,
    load_sem, y_leg_send, y_leg_recv, z_leg_send, z_leg_recv, a_send, a_recv,
    t1_send, t1_recv, t2_send, t2_recv, g_send, g_recv, z_send, z_recv, y_send, y_recv,
):
    n_dp, n_group, piece, span = cfg
    rows = n_dp * piece
    n_y = n_dp // NZ
    unit = span // 4
    relays = (relay_0, relay_1, relay_2, relay_3, relay_4)
    final = len(CHUNKS) - 1
    me = lax.axis_index("dp")
    group = lax.axis_index("group")
    y, z = me // NZ, lax.rem(me, NZ)

    def along_y(j):
        return lax.rem(y + j, n_y)

    def along_z(k):
        return lax.rem(z + k, NZ)

    def remote(source, target, send_sem, recv_sem, place):
        return pltpu.make_async_remote_copy(
            source, target, send_sem, recv_sem, device_id=place, device_id_type=MESH
        )

    barrier = pltpu.get_barrier_semaphore()
    for j in range(1, n_y):
        pl.semaphore_signal(
            barrier, 1, device_id={"dp": along_y(j) * NZ + z}, device_id_type=MESH
        )
    for k in range(1, NZ):
        pl.semaphore_signal(
            barrier, 1, device_id={"dp": y * NZ + along_z(k)}, device_id_type=MESH
        )

    def greet_group(k, c):
        pl.semaphore_signal(
            barrier, 1, device_id={"group": lax.rem(group + k, n_group)}, device_id_type=MESH
        )
        return c

    lax.fori_loop(1, n_group, greet_group, 0)

    pairs = (
        (dest_hbm, dest_ref), (len_hbm, len_ref), (rate_hbm, rate_ref),
        (batch_hbm, batch_ref), (perm_hbm, perm_ref),
    )
    smalls = [pltpu.make_async_copy(a, b, load_sem.at[i]) for i, (a, b) in enumerate(pairs)]
    quarter = n_dp // 4

    def load(q, i):
        source, target = ((r_hbm, rbuf), (v_hbm, vbuf))[q]
        pieces = pl.ds(i * quarter, quarter)
        return pltpu.make_async_copy(
            source.at[pieces], target.at[pieces], load_sem.at[5 + 4 * q + i]
        )

    for copy in smalls:
        copy.start()
    for i in range(4):
        load(0, i).start()
    for i in range(4):
        load(1, i).start()

    for copy in smalls:
        copy.wait()

    def invert(d, c):
        slot = 0
        for p in range(n_dp):
            slot = jnp.where(dest_ref[0, p] == d, p, slot)
        slots_ref[d] = slot
        return c

    lax.fori_loop(0, n_dp, invert, 0)

    for i in range(4):
        load(0, i).wait()

    def gather_r(d, c):
        send_r[d] = rbuf[slots_ref[d]]
        return c

    lax.fori_loop(0, n_dp, gather_r, 0)

    pl.semaphore_wait(barrier, n_y - 1 + NZ - 1 + n_group - 1)

    def y_leg(w, j):
        q, first, width = CHUNKS[w]
        source = (send_r, send_a)[q].at[pl.ds(along_y(j) * NZ, NZ), :, pl.ds(first * unit, width * unit)]
        return remote(
            source, relays[w].at[j - 1], y_leg_send.at[w, j], y_leg_recv.at[w, j],
            {"dp": along_y(j) * NZ + z},
        )

    def z_leg(w, k):
        q, first, width = CHUNKS[w]
        lanes = pl.ds(first * unit, width * unit)
        others = pl.ds(1, n_y - 1)
        target = last.at[others, z] if w == final else (recv_r, recv_a)[q].at[others, z, :, lanes]
        return remote(
            relays[w].at[:, along_z(k)], target, z_leg_send.at[w, k], z_leg_recv.at[w, k],
            {"dp": y * NZ + along_z(k)},
        )

    def straight(p, k):
        q, first, width = STRAIGHT[p]
        source = (send_r, send_a)[q].at[y * NZ + along_z(k), :, pl.ds(first * unit, width * unit)]
        return remote(
            source, (recv_r, recv_a, last)[p].at[0, z], a_send.at[p, k], a_recv.at[p, k],
            {"dp": y * NZ + along_z(k)},
        )

    def start_y_leg(w):
        for j in range(1, n_y):
            y_leg(w, j).start()

    def start_straight(p):
        for k in STEPS:
            straight(p, k).start()

    def forward(w):
        for j in range(1, n_y):
            y_leg(w, j).wait_recv()
        if w == final:
            for place in PLANES:
                k = lax.rem(place - z + NZ, NZ)

                @pl.when(k != 0)
                def _():
                    z_leg(w, k).start()
        else:
            for k in STEPS:
                z_leg(w, k).start()
        q, first, width = CHUNKS[w]
        for j in range(1, n_y):
            if w == final:
                last[j, z] = relays[w][j - 1, z]
            else:
                (recv_r, recv_a)[q][j, z, :, first * unit : (first + width) * unit] = relays[w][j - 1, z]

    start_y_leg(0)
    start_straight(0)
    start_y_leg(1)
    start_y_leg(2)

    for b in range(2):
        for q, ref in enumerate((len_ref, rate_ref)):
            spread = jnp.broadcast_to(column(ref[b : b + 1, :].astype(F32)), (LANES, LANES))
            per = LANES // piece
            cols[q, per * b : per * (b + 1)] = spread.reshape(per, piece, LANES)

    for i in range(4):
        load(1, i).wait()

    def gather_v(d, c):
        p = slots_ref[d]
        vals[d] = vbuf[p]
        sums[0, d] = cols[0, p]
        sums[1, d] = cols[1, p]
        return c

    lax.fori_loop(0, n_dp, gather_v, 0)
    recv_r[0, z] = send_r[me]

    lane = iota((rows, LANES), 1)
    lane_f = lane.astype(F32)
    lengths = sums[0].reshape(rows, LANES).astype(jnp.int32)
    rate = sums[1].reshape(rows, LANES)
    cols[0] = sums[0]
    scales[0] = jnp.exp(-rate)
    scales[1] = jnp.exp(-rate * lane_f)
    scales[2] = jnp.exp(rate * lane_f)
    scales[3] = jnp.exp(-rate * (LANES - lane_f))
    sums[...] = jnp.zeros_like(sums)
    triangle = (iota((LANES, LANES), 0) >= iota((LANES, LANES), 1)).astype(F32)

    def block(i, carry):
        next_head, next_value = carry
        at = span // LANES - 1 - i
        lanes = pl.ds(pl.multiple_of(at * LANES, LANES), LANES)
        position = at * LANES + lane
        length = cols[0].reshape(rows, LANES).astype(jnp.int32)
        reward = send_r[:, :, lanes].astype(F32).reshape(rows, LANES)
        value = vals[:, :, lanes].astype(F32).reshape(rows, LANES)
        valid = position < length
        value_next = jnp.where(lane == LANES - 1, next_value, pltpu.roll(value, LANES - 1, 1))
        value_next = jnp.where(position + 1 < length, value_next, 0.0)
        td = jnp.where(valid, reward + scales[0] * value_next - value, 0.0)
        local = dot(td * scales[1], triangle, precision=HIGHEST) * scales[2]
        total = local + scales[3] * next_head
        rounded = jnp.where(valid, total, 0.0).astype(BF16)
        send_a[:, :, lanes] = rounded.reshape(n_dp, piece, LANES)
        reward = jnp.where(valid, reward, 0.0)
        kept = rounded.astype(F32)
        for q, term in enumerate((reward, kept, reward * reward, kept * kept)):
            sums[q] += term.reshape(n_dp, piece, LANES)
        return total[:, 0:1], value[:, 0:1]

    zero = jnp.zeros((rows, 1), F32)
    third = span // LANES // 3
    carry = lax.fori_loop(0, third, block, (zero, zero))
    forward(0)
    carry = lax.fori_loop(third, 2 * third, block, carry)
    forward(1)
    lax.fori_loop(2 * third, span // LANES, block, carry)
    recv_a[0, z] = send_a[me, :, 0 : span // 2]
    last[0, z] = send_a[me, :, span // 2 : span]

    term_of, row_of = lane // piece, lax.rem(lane, piece)
    own = row_of == lax.rem(iota((rows, LANES), 0), piece)
    packed = jnp.where(own & (term_of == 0), cols[0].reshape(rows, LANES), 0.0)
    for q in range(4):
        total = jnp.sum(sums[q].reshape(rows, LANES), axis=1, keepdims=True)
        packed = jnp.where(own & (term_of == q + 1), total, packed)
    tsend[...] = jnp.sum(packed.reshape(n_dp, piece, LANES), axis=1, keepdims=True)

    for b in range(2):
        here = slice(b * LANES, (b + 1) * LANES)
        order = column(perm_ref[b : b + 1, :].astype(F32)).astype(jnp.int32)
        chooser[b] = (order == iota((LANES, LANES), 1)).astype(BF16)
        batch = column(batch_ref[b : b + 1, :].astype(F32)).astype(jnp.int32)
        member[here] = (batch == iota((LANES, LANES), 1)).astype(F32)

    def terms_y(j):
        return remote(
            tsend.at[pl.ds(along_y(j) * NZ, NZ)], trelay.at[j], t1_send.at[j], t1_recv.at[j],
            {"dp": along_y(j) * NZ + z},
        )

    def terms_z(k):
        return remote(
            trelay.at[:, along_z(k)], trecv.at[:, z], t2_send.at[k], t2_recv.at[k],
            {"dp": y * NZ + along_z(k)},
        )

    trelay[0] = tsend[pl.ds(y * NZ, NZ)]
    for j in range(1, n_y):
        terms_y(j).start()
    start_y_leg(3)
    start_y_leg(4)
    for j in range(1, n_y):
        terms_y(j).wait()
    for k in STEPS:
        terms_z(k).start()
    forward(2)
    trecv[:, z] = trelay[:, z]
    for k in STEPS:
        terms_z(k).wait()

    ordered = [trecv[lax.rem(y - h + n_y, n_y)] for h in range(n_y)]
    spread = jnp.concatenate(ordered, axis=0)
    spread = jnp.broadcast_to(spread, (n_dp, piece, LANES)).reshape(rows, LANES)
    spread = jnp.where(own, spread, 0.0)
    select = (iota((LANES, LANES), 0) // piece == iota((LANES, LANES), 1)).astype(F32)
    totals = jnp.zeros((LANES, LANES), F32)
    for b in range(2):
        here = slice(b * LANES, (b + 1) * LANES)
        moved = dot(chooser[b].astype(F32), spread[here], precision=HIGHEST)
        moved = dot(moved, select, precision=HIGHEST)
        stats[2, here] = jnp.broadcast_to(moved[:, 0:1], (LANES, LANES))
        totals += dot(moved, member[here], (((0,), (0,)), ((), ())), precision=HIGHEST)

    def exchange(store, index, sizes, target, send_sem, recv_sem, between):
        store[index] = part[...]

        def copy(k):
            return pltpu.make_async_remote_copy(
                part, store.at[index], send_sem.at[k], recv_sem.at[k],
                device_id=target(k), device_id_type=MESH,
            )

        def go(k, c):
            copy(k).start()
            return c

        def done(k, c):
            copy(k).wait()
            return c

        lax.fori_loop(1, sizes, go, 0)
        between()
        lax.fori_loop(1, sizes, done, 0)
        part[...] = jnp.sum(store[...], axis=0)

    part[...] = totals[0:8]
    exchange(
        st_g, group, n_group, lambda k: {"group": lax.rem(group + k, n_group)},
        g_send, g_recv, lambda: None,
    )
    def advantage_straight():
        start_straight(1)
        start_straight(2)
        forward(3)

    exchange(
        st_z, z, NZ, lambda k: {"dp": y * NZ + along_z(k)}, z_send, z_recv, advantage_straight
    )
    exchange(
        st_y, y, n_y, lambda k: {"dp": along_y(k) * NZ + z}, y_send, y_recv, lambda: forward(final)
    )

    total = part[...]
    count = jnp.maximum(total[0:1], 1.0)
    for q in range(2):
        mean = total[1 + q : 2 + q] / count
        spread = total[3 + q : 4 + q] / count - mean * mean
        for s, value in enumerate((mean, lax.rsqrt(spread + 1e-05))):
            picked = jnp.sum(member[...] * value, axis=1, keepdims=True)
            (stats_r, stats)[q][s] = jnp.broadcast_to(picked, (rows, LANES))

    tile = 256
    for w, (q, first, width) in enumerate(CHUNKS):
        for p, (kind, begin, _) in enumerate(STRAIGHT):
            if (kind, begin) == (q, first):
                for k in STEPS:
                    straight(p, k).wait()
        for k in STEPS:
            z_leg(w, k).wait()
        if w == final:
            break
        source, out, moments = ((recv_r, out_r, stats_r), (recv_a, out_a, stats))[q]

        def finish(i, c):
            start = pl.multiple_of(first * unit + i * tile, LANES)
            for b in range(2):
                here = slice(b * LANES, (b + 1) * LANES)
                out[here, pl.ds(start, tile)] = whiten(
                    source, y, b, pl.ds(start, tile), chooser[b],
                    moments[0, here], moments[1, here], stats[2, here].astype(jnp.int32), start,
                )
            return c

        lax.fori_loop(0, width * unit // tile, finish, 0)
    for w in range(len(CHUNKS)):
        for j in range(1, n_y):
            y_leg(w, j).wait_send()


def finish_kernel(n_dp, white_r, white_a, last, chooser, stats, out_r, out_a, white, sem):
    rows, width = white.shape
    ready = white_a.shape[1]
    y = lax.axis_index("dp") // NZ
    copies = []

    def send(source, target):
        copy = pltpu.make_async_copy(source, target, sem.at[len(copies)])
        copy.start()
        copies.append(copy)

    for i in range(4):
        here = pl.ds(i * (rows // 4), rows // 4)
        send(white_r.at[here], out_r.at[here])
        send(white_a.at[here], out_a.at[here, 0:ready])
    tile = 512
    for i in range(width // tile):
        lanes = slice(i * tile, (i + 1) * tile)
        for b in range(2):
            here = slice(b * LANES, (b + 1) * LANES)
            white[here, lanes] = whiten(
                last, y, b, lanes, chooser[b],
                stats[0, here], stats[1, here], stats[2, here].astype(jnp.int32), ready + i * tile,
            )
        send(white.at[:, lanes], out_a.at[:, ready + i * tile : ready + (i + 1) * tile])
    for copy in copies:
        copy.wait()


def local(rewards, values, lengths, decay_rate, piece_dest, row_perm, minibatch, *, n_dp, n_group):
    rows, span = rewards.shape
    piece = rows // n_dp
    half = span // 2
    unit = span // 4
    n_y = n_dp // NZ
    vmem = pl.BlockSpec(memory_space=pltpu.VMEM)
    hbm = pl.BlockSpec(memory_space=pltpu.HBM)
    bulk = pltpu.VMEM((n_dp, piece, span), BF16)
    dma = pltpu.SemaphoreType.DMA
    chunks = len(CHUNKS)
    result = jax.ShapeDtypeStruct((rows, span), BF16)
    parts = pl.pallas_call(
        functools.partial(kernel, (n_dp, n_group, piece, span)),
        out_shape=(
            result,
            jax.ShapeDtypeStruct((rows, half), BF16),
            jax.ShapeDtypeStruct((n_y, NZ, piece, half), BF16),
            jax.ShapeDtypeStruct((2, LANES, LANES), BF16),
            jax.ShapeDtypeStruct((3, rows, LANES), F32),
        ),
        in_specs=[hbm] * 7,
        out_specs=(vmem,) * 5,
        scratch_shapes=[
            pltpu.SMEM((1, n_dp), jnp.int32),
            pltpu.SMEM((n_dp,), jnp.int32),
            pltpu.VMEM((2, LANES), jnp.int32),
            pltpu.VMEM((2, LANES), F32),
            pltpu.VMEM((2, LANES), jnp.int32),
            pltpu.VMEM((2, LANES), jnp.int32),
        ]
        + [bulk] * 5
        + [
            pltpu.VMEM((n_y, NZ, piece, span), BF16),
            pltpu.VMEM((n_y, NZ, piece, half), BF16),
        ]
        + [pltpu.VMEM((n_y - 1, NZ, piece, w * unit), BF16) for _, _, w in CHUNKS]
        + [
            pltpu.VMEM((2, n_dp, piece, LANES), F32),
            pltpu.VMEM((4, rows, LANES), F32),
            pltpu.VMEM((4, n_dp, piece, LANES), F32),
            pltpu.VMEM((rows, LANES), F32),
            pltpu.VMEM((2, rows, LANES), F32),
            pltpu.VMEM((n_dp, 1, LANES), F32),
            pltpu.VMEM((n_y, NZ, 1, LANES), F32),
            pltpu.VMEM((n_y, NZ, 1, LANES), F32),
            pltpu.VMEM((8, LANES), F32),
            pltpu.VMEM((NZ, 8, LANES), F32),
            pltpu.VMEM((n_y, 8, LANES), F32),
            pltpu.VMEM((n_group, 8, LANES), F32),
            dma((13,)),
            dma((chunks, n_y)), dma((chunks, n_y)),
            dma((chunks, NZ)), dma((chunks, NZ)),
            dma((len(STRAIGHT), NZ)), dma((len(STRAIGHT), NZ)),
            dma((n_y,)), dma((n_y,)),
            dma((NZ,)), dma((NZ,)),
            dma((n_group,)), dma((n_group,)),
            dma((NZ,)), dma((NZ,)),
            dma((n_y,)), dma((n_y,)),
        ],
        compiler_params=pltpu.CompilerParams(
            collective_id=0, has_side_effects=True, vmem_limit_bytes=40 * 2**20
        ),
        name="reshuffle",
    )(
        *(
            pltpu.with_memory_space_constraint(array, pltpu.HBM)
            for array in (
                piece_dest,
                lengths.reshape(2, LANES),
                decay_rate.reshape(2, LANES),
                minibatch.reshape(2, LANES),
                row_perm,
                rewards.reshape(n_dp, piece, span),
                values.reshape(n_dp, piece, span),
            )
        )
    )
    return pl.pallas_call(
        functools.partial(finish_kernel, n_dp),
        out_shape=(result, result),
        in_specs=[vmem] * 5,
        out_specs=(hbm, hbm),
        scratch_shapes=[pltpu.VMEM((rows, half), BF16), dma((12,))],
        compiler_params=pltpu.CompilerParams(vmem_limit_bytes=16 * 2**20),
        name="finish",
    )(*parts)


def solution(mesh):
    both = ("dp", "group")
    return jax.shard_map(
        functools.partial(local, n_dp=mesh.shape["dp"], n_group=mesh.shape["group"]),
        mesh=mesh,
        in_specs=(
            P(both, None), P(both, None), P(both), P(both), P("dp", None), P(both, None), P(both),
        ),
        out_specs=(P(both, None), P(both, None)),
        check_vma=False,
    )
```

```python
import functools

import jax
import jax.numpy as jnp
from jax import lax
from jax.experimental import pallas as pl
from jax.experimental.pallas import tpu as pltpu
from jax.sharding import PartitionSpec as P

MESH = pl.DeviceIdType.MESH
HIGHEST = lax.Precision.HIGHEST
F32 = jnp.float32
BF16 = jnp.bfloat16
LANES = 128
NZ = 8
CHUNKS = ((0, 0, 1), (0, 1, 1), (0, 2, 2), (1, 0, 2), (1, 2, 2))
STRAIGHT = ((0, 0, 4), (1, 0, 2), (1, 2, 2))
STEPS = (4, 3, 5, 2, 6, 1, 7)
PLANES = (0, 1, 2, 3, 7, 4, 6, 5)


def dot(a, b, dims=(((1,), (0,)), ((), ())), precision=None):
    return lax.dot_general(a, b, dims, precision=precision, preferred_element_type=F32)


def iota(shape, dim):
    return lax.broadcasted_iota(jnp.int32, shape, dim)


def column(row):
    on = iota((LANES, LANES), 0) == iota((LANES, LANES), 1)
    return jnp.sum(jnp.where(on, row, 0.0), axis=1, keepdims=True)


def whiten(source, y, b, lanes, chooser, mean, scale, length, start):
    n_y = source.shape[0]
    half = n_y // 2
    pieces = [source[lax.rem(y - b * half - h + n_y, n_y), :, :, lanes] for h in range(half)]
    block = jnp.concatenate([p.astype(F32) for p in pieces], axis=0)
    tile = block.shape[-1]
    moved = dot(chooser, block.reshape(LANES, tile).astype(BF16))
    done = []
    for s in range(tile // LANES):
        position = start + s * LANES + iota((LANES, LANES), 1)
        white = (moved[:, s * LANES : (s + 1) * LANES] - mean) * scale
        done.append(jnp.where(position < length, white, 0.0).astype(BF16))
    return jnp.concatenate(done, axis=1)


def kernel(
    cfg, dest_hbm, len_hbm, rate_hbm, batch_hbm, perm_hbm, r_hbm, v_hbm,
    out_r, out_a, last, chooser, stats,
    dest_ref, slots_ref, len_ref, rate_ref, batch_ref, perm_ref, rbuf, vbuf, send_r, send_a, vals, recv_r, recv_a,
    relay_0, relay_1, relay_2, relay_3, relay_4,
    cols, scales, sums, member, stats_r, tsend, trelay, trecv, part, st_z, st_y, st_g,
    load_sem, y_leg_send, y_leg_recv, z_leg_send, z_leg_recv, a_send, a_recv,
    t1_send, t1_recv, t2_send, t2_recv, g_send, g_recv, z_send, z_recv, y_send, y_recv,
):
    n_dp, n_group, piece, span = cfg
    rows = n_dp * piece
    n_y = n_dp // NZ
    unit = span // 4
    relays = (relay_0, relay_1, relay_2, relay_3, relay_4)
    final = len(CHUNKS) - 1
    me = lax.axis_index("dp")
    group = lax.axis_index("group")
    y, z = me // NZ, lax.rem(me, NZ)

    def along_y(j):
        return lax.rem(y + j, n_y)

    def along_z(k):
        return lax.rem(z + k, NZ)

    def remote(source, target, send_sem, recv_sem, place):
        return pltpu.make_async_remote_copy(
            source, target, send_sem, recv_sem, device_id=place, device_id_type=MESH
        )

    barrier = pltpu.get_barrier_semaphore()
    for j in range(1, n_y):
        pl.semaphore_signal(
            barrier, 1, device_id={"dp": along_y(j) * NZ + z}, device_id_type=MESH
        )
    for k in range(1, NZ):
        pl.semaphore_signal(
            barrier, 1, device_id={"dp": y * NZ + along_z(k)}, device_id_type=MESH
        )

    def greet_group(k, c):
        pl.semaphore_signal(
            barrier, 1, device_id={"group": lax.rem(group + k, n_group)}, device_id_type=MESH
        )
        return c

    lax.fori_loop(1, n_group, greet_group, 0)

    pairs = (
        (dest_hbm, dest_ref), (len_hbm, len_ref), (rate_hbm, rate_ref),
        (batch_hbm, batch_ref), (perm_hbm, perm_ref),
    )
    smalls = [pltpu.make_async_copy(a, b, load_sem.at[i]) for i, (a, b) in enumerate(pairs)]
    quarter = n_dp // 4

    def load(q, i):
        source, target = ((r_hbm, rbuf), (v_hbm, vbuf))[q]
        pieces = pl.ds(i * quarter, quarter)
        return pltpu.make_async_copy(
            source.at[pieces], target.at[pieces], load_sem.at[5 + 4 * q + i]
        )

    for copy in smalls:
        copy.start()
    for i in range(4):
        load(0, i).start()
    for i in range(4):
        load(1, i).start()

    for copy in smalls:
        copy.wait()

    def invert(d, c):
        slot = 0
        for p in range(n_dp):
            slot = jnp.where(dest_ref[0, p] == d, p, slot)
        slots_ref[d] = slot
        return c

    lax.fori_loop(0, n_dp, invert, 0)

    for i in range(4):
        load(0, i).wait()

    def gather_r(d, c):
        send_r[d] = rbuf[slots_ref[d]]
        return c

    lax.fori_loop(0, n_dp, gather_r, 0)

    pl.semaphore_wait(barrier, n_y - 1 + NZ - 1 + n_group - 1)

    def y_leg(w, j):
        q, first, width = CHUNKS[w]
        source = (send_r, send_a)[q].at[pl.ds(along_y(j) * NZ, NZ), :, pl.ds(first * unit, width * unit)]
        return remote(
            source, relays[w].at[j - 1], y_leg_send.at[w, j], y_leg_recv.at[w, j],
            {"dp": along_y(j) * NZ + z},
        )

    def z_leg(w, k):
        q, first, width = CHUNKS[w]
        lanes = pl.ds(first * unit, width * unit)
        others = pl.ds(1, n_y - 1)
        target = last.at[others, z] if w == final else (recv_r, recv_a)[q].at[others, z, :, lanes]
        return remote(
            relays[w].at[:, along_z(k)], target, z_leg_send.at[w, k], z_leg_recv.at[w, k],
            {"dp": y * NZ + along_z(k)},
        )

    def straight(p, k):
        q, first, width = STRAIGHT[p]
        source = (send_r, send_a)[q].at[y * NZ + along_z(k), :, pl.ds(first * unit, width * unit)]
        return remote(
            source, (recv_r, recv_a, last)[p].at[0, z], a_send.at[p, k], a_recv.at[p, k],
            {"dp": y * NZ + along_z(k)},
        )

    def start_y_leg(w):
        for j in range(1, n_y):
            y_leg(w, j).start()

    def start_straight(p):
        for k in STEPS:
            straight(p, k).start()

    def forward(w):
        for j in range(1, n_y):
            y_leg(w, j).wait_recv()
        if w == final:
            for place in PLANES:
                k = lax.rem(place - z + NZ, NZ)

                @pl.when(k != 0)
                def _():
                    z_leg(w, k).start()
        else:
            for k in STEPS:
                z_leg(w, k).start()
        q, first, width = CHUNKS[w]
        for j in range(1, n_y):
            if w == final:
                last[j, z] = relays[w][j - 1, z]
            else:
                (recv_r, recv_a)[q][j, z, :, first * unit : (first + width) * unit] = relays[w][j - 1, z]

    start_y_leg(0)
    start_straight(0)
    start_y_leg(1)
    start_y_leg(2)

    for b in range(2):
        for q, ref in enumerate((len_ref, rate_ref)):
            spread = jnp.broadcast_to(column(ref[b : b + 1, :].astype(F32)), (LANES, LANES))
            per = LANES // piece
            cols[q, per * b : per * (b + 1)] = spread.reshape(per, piece, LANES)

    for i in range(4):
        load(1, i).wait()

    def gather_v(d, c):
        p = slots_ref[d]
        vals[d] = vbuf[p]
        sums[0, d] = cols[0, p]
        sums[1, d] = cols[1, p]
        return c

    lax.fori_loop(0, n_dp, gather_v, 0)
    recv_r[0, z] = send_r[me]

    lane = iota((rows, LANES), 1)
    lane_f = lane.astype(F32)
    lengths = sums[0].reshape(rows, LANES).astype(jnp.int32)
    rate = sums[1].reshape(rows, LANES)
    cols[0] = sums[0]
    scales[0] = jnp.exp(-rate)
    scales[1] = jnp.exp(-rate * lane_f)
    scales[2] = jnp.exp(rate * lane_f)
    scales[3] = jnp.exp(-rate * (LANES - lane_f))
    sums[...] = jnp.zeros_like(sums)
    triangle = (iota((LANES, LANES), 0) >= iota((LANES, LANES), 1)).astype(F32)

    def block(i, carry):
        next_head, next_value = carry
        at = span // LANES - 1 - i
        lanes = pl.ds(pl.multiple_of(at * LANES, LANES), LANES)
        position = at * LANES + lane
        length = cols[0].reshape(rows, LANES).astype(jnp.int32)
        reward = send_r[:, :, lanes].astype(F32).reshape(rows, LANES)
        value = vals[:, :, lanes].astype(F32).reshape(rows, LANES)
        valid = position < length
        value_next = jnp.where(lane == LANES - 1, next_value, pltpu.roll(value, LANES - 1, 1))
        value_next = jnp.where(position + 1 < length, value_next, 0.0)
        td = jnp.where(valid, reward + scales[0] * value_next - value, 0.0)
        local = dot(td * scales[1], triangle, precision=HIGHEST) * scales[2]
        total = local + scales[3] * next_head
        rounded = jnp.where(valid, total, 0.0).astype(BF16)
        send_a[:, :, lanes] = rounded.reshape(n_dp, piece, LANES)
        reward = jnp.where(valid, reward, 0.0)
        kept = rounded.astype(F32)
        for q, term in enumerate((reward, kept, reward * reward, kept * kept)):
            sums[q] += term.reshape(n_dp, piece, LANES)
        return total[:, 0:1], value[:, 0:1]

    zero = jnp.zeros((rows, 1), F32)
    third = span // LANES // 3
    carry = lax.fori_loop(0, third, block, (zero, zero))
    forward(0)
    carry = lax.fori_loop(third, 2 * third, block, carry)
    forward(1)
    lax.fori_loop(2 * third, span // LANES, block, carry)
    recv_a[0, z] = send_a[me, :, 0 : span // 2]
    last[0, z] = send_a[me, :, span // 2 : span]

    term_of, row_of = lane // piece, lax.rem(lane, piece)
    own = row_of == lax.rem(iota((rows, LANES), 0), piece)
    packed = jnp.where(own & (term_of == 0), cols[0].reshape(rows, LANES), 0.0)
    for q in range(4):
        total = jnp.sum(sums[q].reshape(rows, LANES), axis=1, keepdims=True)
        packed = jnp.where(own & (term_of == q + 1), total, packed)
    tsend[...] = jnp.sum(packed.reshape(n_dp, piece, LANES), axis=1, keepdims=True)

    for b in range(2):
        here = slice(b * LANES, (b + 1) * LANES)
        order = column(perm_ref[b : b + 1, :].astype(F32)).astype(jnp.int32)
        chooser[b] = (order == iota((LANES, LANES), 1)).astype(BF16)
        batch = column(batch_ref[b : b + 1, :].astype(F32)).astype(jnp.int32)
        member[here] = (batch == iota((LANES, LANES), 1)).astype(F32)

    def terms_y(j):
        return remote(
            tsend.at[pl.ds(along_y(j) * NZ, NZ)], trelay.at[j], t1_send.at[j], t1_recv.at[j],
            {"dp": along_y(j) * NZ + z},
        )

    def terms_z(k):
        return remote(
            trelay.at[:, along_z(k)], trecv.at[:, z], t2_send.at[k], t2_recv.at[k],
            {"dp": y * NZ + along_z(k)},
        )

    trelay[0] = tsend[pl.ds(y * NZ, NZ)]
    for j in range(1, n_y):
        terms_y(j).start()
    start_y_leg(3)
    start_y_leg(4)
    for j in range(1, n_y):
        terms_y(j).wait()
    for k in STEPS:
        terms_z(k).start()
    forward(2)
    trecv[:, z] = trelay[:, z]
    for k in STEPS:
        terms_z(k).wait()

    ordered = [trecv[lax.rem(y - h + n_y, n_y)] for h in range(n_y)]
    spread = jnp.concatenate(ordered, axis=0)
    spread = jnp.broadcast_to(spread, (n_dp, piece, LANES)).reshape(rows, LANES)
    spread = jnp.where(own, spread, 0.0)
    select = (iota((LANES, LANES), 0) // piece == iota((LANES, LANES), 1)).astype(F32)
    totals = jnp.zeros((LANES, LANES), F32)
    for b in range(2):
        here = slice(b * LANES, (b + 1) * LANES)
        moved = dot(chooser[b].astype(F32), spread[here], precision=HIGHEST)
        moved = dot(moved, select, precision=HIGHEST)
        stats[2, here] = jnp.broadcast_to(moved[:, 0:1], (LANES, LANES))
        totals += dot(moved, member[here], (((0,), (0,)), ((), ())), precision=HIGHEST)

    def exchange(store, index, sizes, target, send_sem, recv_sem, between):
        store[index] = part[...]

        def copy(k):
            return pltpu.make_async_remote_copy(
                part, store.at[index], send_sem.at[k], recv_sem.at[k],
                device_id=target(k), device_id_type=MESH,
            )

        def go(k, c):
            copy(k).start()
            return c

        def done(k, c):
            copy(k).wait()
            return c

        lax.fori_loop(1, sizes, go, 0)
        between()
        lax.fori_loop(1, sizes, done, 0)
        part[...] = jnp.sum(store[...], axis=0)

    part[...] = totals[0:8]
    exchange(
        st_g, group, n_group, lambda k: {"group": lax.rem(group + k, n_group)},
        g_send, g_recv, lambda: None,
    )
    def advantage_straight():
        start_straight(1)
        start_straight(2)
        forward(3)

    exchange(
        st_z, z, NZ, lambda k: {"dp": y * NZ + along_z(k)}, z_send, z_recv, advantage_straight
    )
    exchange(
        st_y, y, n_y, lambda k: {"dp": along_y(k) * NZ + z}, y_send, y_recv, lambda: forward(final)
    )

    total = part[...]
    count = jnp.maximum(total[0:1], 1.0)
    for q in range(2):
        mean = total[1 + q : 2 + q] / count
        spread = jnp.maximum(total[3 + q : 4 + q] / count - mean * mean, 0.0)
        for s, value in enumerate((mean, lax.rsqrt(spread + 1e-05))):
            picked = jnp.sum(member[...] * value, axis=1, keepdims=True)
            (stats_r, stats)[q][s] = jnp.broadcast_to(picked, (rows, LANES))

    tile = 256
    for w, (q, first, width) in enumerate(CHUNKS):
        for p, (kind, begin, _) in enumerate(STRAIGHT):
            if (kind, begin) == (q, first):
                for k in STEPS:
                    straight(p, k).wait()
        for k in STEPS:
            z_leg(w, k).wait()
        if w == final:
            break
        source, out, moments = ((recv_r, out_r, stats_r), (recv_a, out_a, stats))[q]

        def finish(i, c):
            start = pl.multiple_of(first * unit + i * tile, LANES)
            for b in range(2):
                here = slice(b * LANES, (b + 1) * LANES)
                out[here, pl.ds(start, tile)] = whiten(
                    source, y, b, pl.ds(start, tile), chooser[b],
                    moments[0, here], moments[1, here], stats[2, here].astype(jnp.int32), start,
                )
            return c

        lax.fori_loop(0, width * unit // tile, finish, 0)
    for w in range(len(CHUNKS)):
        for j in range(1, n_y):
            y_leg(w, j).wait_send()


def finish_kernel(n_dp, white_r, white_a, last, chooser, stats, out_r, out_a, white, sem):
    rows, width = white.shape
    ready = white_a.shape[1]
    y = lax.axis_index("dp") // NZ
    copies = []

    def send(source, target):
        copy = pltpu.make_async_copy(source, target, sem.at[len(copies)])
        copy.start()
        copies.append(copy)

    for i in range(4):
        here = pl.ds(i * (rows // 4), rows // 4)
        send(white_r.at[here], out_r.at[here])
        send(white_a.at[here], out_a.at[here, 0:ready])
    tile = 512
    for i in range(width // tile):
        lanes = slice(i * tile, (i + 1) * tile)
        for b in range(2):
            here = slice(b * LANES, (b + 1) * LANES)
            white[here, lanes] = whiten(
                last, y, b, lanes, chooser[b],
                stats[0, here], stats[1, here], stats[2, here].astype(jnp.int32), ready + i * tile,
            )
        send(white.at[:, lanes], out_a.at[:, ready + i * tile : ready + (i + 1) * tile])
    for copy in copies:
        copy.wait()


def local(rewards, values, lengths, decay_rate, piece_dest, row_perm, minibatch, *, n_dp, n_group):
    rows, span = rewards.shape
    piece = rows // n_dp
    half = span // 2
    unit = span // 4
    n_y = n_dp // NZ
    vmem = pl.BlockSpec(memory_space=pltpu.VMEM)
    hbm = pl.BlockSpec(memory_space=pltpu.HBM)
    bulk = pltpu.VMEM((n_dp, piece, span), BF16)
    dma = pltpu.SemaphoreType.DMA
    chunks = len(CHUNKS)
    result = jax.ShapeDtypeStruct((rows, span), BF16)
    parts = pl.pallas_call(
        functools.partial(kernel, (n_dp, n_group, piece, span)),
        out_shape=(
            result,
            jax.ShapeDtypeStruct((rows, half), BF16),
            jax.ShapeDtypeStruct((n_y, NZ, piece, half), BF16),
            jax.ShapeDtypeStruct((2, LANES, LANES), BF16),
            jax.ShapeDtypeStruct((3, rows, LANES), F32),
        ),
        in_specs=[hbm] * 7,
        out_specs=(vmem,) * 5,
        scratch_shapes=[
            pltpu.SMEM((1, n_dp), jnp.int32),
            pltpu.SMEM((n_dp,), jnp.int32),
            pltpu.VMEM((2, LANES), jnp.int32),
            pltpu.VMEM((2, LANES), F32),
            pltpu.VMEM((2, LANES), jnp.int32),
            pltpu.VMEM((2, LANES), jnp.int32),
        ]
        + [bulk] * 5
        + [
            pltpu.VMEM((n_y, NZ, piece, span), BF16),
            pltpu.VMEM((n_y, NZ, piece, half), BF16),
        ]
        + [pltpu.VMEM((n_y - 1, NZ, piece, w * unit), BF16) for _, _, w in CHUNKS]
        + [
            pltpu.VMEM((2, n_dp, piece, LANES), F32),
            pltpu.VMEM((4, rows, LANES), F32),
            pltpu.VMEM((4, n_dp, piece, LANES), F32),
            pltpu.VMEM((rows, LANES), F32),
            pltpu.VMEM((2, rows, LANES), F32),
            pltpu.VMEM((n_dp, 1, LANES), F32),
            pltpu.VMEM((n_y, NZ, 1, LANES), F32),
            pltpu.VMEM((n_y, NZ, 1, LANES), F32),
            pltpu.VMEM((8, LANES), F32),
            pltpu.VMEM((NZ, 8, LANES), F32),
            pltpu.VMEM((n_y, 8, LANES), F32),
            pltpu.VMEM((n_group, 8, LANES), F32),
            dma((13,)),
            dma((chunks, n_y)), dma((chunks, n_y)),
            dma((chunks, NZ)), dma((chunks, NZ)),
            dma((len(STRAIGHT), NZ)), dma((len(STRAIGHT), NZ)),
            dma((n_y,)), dma((n_y,)),
            dma((NZ,)), dma((NZ,)),
            dma((n_group,)), dma((n_group,)),
            dma((NZ,)), dma((NZ,)),
            dma((n_y,)), dma((n_y,)),
        ],
        compiler_params=pltpu.CompilerParams(
            collective_id=0, has_side_effects=True, vmem_limit_bytes=40 * 2**20
        ),
        name="reshuffle",
    )(
        *(
            pltpu.with_memory_space_constraint(array, pltpu.HBM)
            for array in (
                piece_dest,
                lengths.reshape(2, LANES),
                decay_rate.reshape(2, LANES),
                minibatch.reshape(2, LANES),
                row_perm,
                rewards.reshape(n_dp, piece, span),
                values.reshape(n_dp, piece, span),
            )
        )
    )
    return pl.pallas_call(
        functools.partial(finish_kernel, n_dp),
        out_shape=(result, result),
        in_specs=[vmem] * 5,
        out_specs=(hbm, hbm),
        scratch_shapes=[pltpu.VMEM((rows, half), BF16), dma((12,))],
        compiler_params=pltpu.CompilerParams(vmem_limit_bytes=16 * 2**20),
        name="finish",
    )(*parts)


def solution(mesh):
    both = ("dp", "group")
    return jax.shard_map(
        functools.partial(local, n_dp=mesh.shape["dp"], n_group=mesh.shape["group"]),
        mesh=mesh,
        in_specs=(
            P(both, None), P(both, None), P(both), P(both), P("dp", None), P(both, None), P(both),
        ),
        out_specs=(P(both, None), P(both, None)),
        check_vma=False,
    )
```

```python
import functools

import jax
import jax.numpy as jnp
from jax import lax
from jax.experimental import pallas as pl
from jax.experimental.pallas import tpu as pltpu
from jax.sharding import PartitionSpec as P

MESH = pl.DeviceIdType.MESH
HIGHEST = lax.Precision.HIGHEST
F32 = jnp.float32
BF16 = jnp.bfloat16
LANES = 128
NZ = 8
CHUNKS = ((0, 0, 1), (0, 1, 1), (0, 2, 2), (1, 0, 2), (1, 2, 2))
STRAIGHT = ((0, 0, 4), (1, 0, 2), (1, 2, 2))
STEPS = (4, 3, 5, 2, 6, 1, 7)
PLANES = (0, 1, 2, 3, 7, 4, 6, 5)


def dot(a, b, dims=(((1,), (0,)), ((), ())), precision=None):
    return lax.dot_general(a, b, dims, precision=precision, preferred_element_type=F32)


def iota(shape, dim):
    return lax.broadcasted_iota(jnp.int32, shape, dim)


def column(row):
    on = iota((LANES, LANES), 0) == iota((LANES, LANES), 1)
    return jnp.sum(jnp.where(on, row, 0.0), axis=1, keepdims=True)


def whiten(source, y, b, lanes, chooser, mean, scale, length, start):
    n_y = source.shape[0]
    half = n_y // 2
    pieces = [source[lax.rem(y - b * half - h + n_y, n_y), :, :, lanes] for h in range(half)]
    block = jnp.concatenate([p.astype(F32) for p in pieces], axis=0)
    tile = block.shape[-1]
    moved = dot(chooser, block.reshape(LANES, tile).astype(BF16))
    done = []
    for s in range(tile // LANES):
        position = start + s * LANES + iota((LANES, LANES), 1)
        white = (moved[:, s * LANES : (s + 1) * LANES] - mean) * scale
        done.append(jnp.where(position < length, white, 0.0).astype(BF16))
    return jnp.concatenate(done, axis=1)


def kernel(
    cfg, dest_hbm, len_hbm, rate_hbm, batch_hbm, perm_hbm, r_hbm, v_hbm,
    out_r, out_a, last, chooser, stats,
    dest_ref, slots_ref, len_ref, rate_ref, batch_ref, perm_ref, rbuf, vbuf, send_r, send_a, vals, recv_r, recv_a,
    relay_0, relay_1, relay_2, relay_3, relay_4,
    cols, scales, sums, member, stats_r, tsend, trelay, trecv, part, st_z, st_y, st_g,
    load_sem, y_leg_send, y_leg_recv, z_leg_send, z_leg_recv, a_send, a_recv,
    t1_send, t1_recv, t2_send, t2_recv, g_send, g_recv, z_send, z_recv, y_send, y_recv,
):
    n_dp, n_group, piece, span = cfg
    rows = n_dp * piece
    n_y = n_dp // NZ
    unit = span // 4
    relays = (relay_0, relay_1, relay_2, relay_3, relay_4)
    final = len(CHUNKS) - 1
    me = lax.axis_index("dp")
    group = lax.axis_index("group")
    y, z = me // NZ, lax.rem(me, NZ)

    def along_y(j):
        return lax.rem(y + j, n_y)

    def along_z(k):
        return lax.rem(z + k, NZ)

    def remote(source, target, send_sem, recv_sem, place):
        return pltpu.make_async_remote_copy(
            source, target, send_sem, recv_sem, device_id=place, device_id_type=MESH
        )

    barrier = pltpu.get_barrier_semaphore()
    for j in range(1, n_y):
        pl.semaphore_signal(
            barrier, 1, device_id={"dp": along_y(j) * NZ + z}, device_id_type=MESH
        )
    for k in range(1, NZ):
        pl.semaphore_signal(
            barrier, 1, device_id={"dp": y * NZ + along_z(k)}, device_id_type=MESH
        )

    def greet_group(k, c):
        pl.semaphore_signal(
            barrier, 1, device_id={"group": lax.rem(group + k, n_group)}, device_id_type=MESH
        )
        return c

    lax.fori_loop(1, n_group, greet_group, 0)

    pairs = (
        (dest_hbm, dest_ref), (len_hbm, len_ref), (rate_hbm, rate_ref),
        (batch_hbm, batch_ref), (perm_hbm, perm_ref),
    )
    smalls = [pltpu.make_async_copy(a, b, load_sem.at[i]) for i, (a, b) in enumerate(pairs)]
    quarter = n_dp // 4

    def load(q, i):
        source, target = ((r_hbm, rbuf), (v_hbm, vbuf))[q]
        pieces = pl.ds(i * quarter, quarter)
        return pltpu.make_async_copy(
            source.at[pieces], target.at[pieces], load_sem.at[5 + 4 * q + i]
        )

    for copy in smalls:
        copy.start()
    for i in range(4):
        load(0, i).start()
    for i in range(4):
        load(1, i).start()

    for copy in smalls:
        copy.wait()

    def invert(d, c):
        slot = 0
        for p in range(n_dp):
            slot = jnp.where(dest_ref[0, p] == d, p, slot)
        slots_ref[d] = slot
        return c

    lax.fori_loop(0, n_dp, invert, 0)

    for i in range(4):
        load(0, i).wait()

    def gather_r(d, c):
        send_r[d] = rbuf[slots_ref[d]]
        return c

    lax.fori_loop(0, n_dp, gather_r, 0)

    pl.semaphore_wait(barrier, n_y - 1 + NZ - 1 + n_group - 1)

    def y_leg(w, j):
        q, first, width = CHUNKS[w]
        source = (send_r, send_a)[q].at[pl.ds(along_y(j) * NZ, NZ), :, pl.ds(first * unit, width * unit)]
        return remote(
            source, relays[w].at[j - 1], y_leg_send.at[w, j], y_leg_recv.at[w, j],
            {"dp": along_y(j) * NZ + z},
        )

    def z_leg(w, k):
        q, first, width = CHUNKS[w]
        lanes = pl.ds(first * unit, width * unit)
        others = pl.ds(1, n_y - 1)
        target = last.at[others, z] if w == final else (recv_r, recv_a)[q].at[others, z, :, lanes]
        return remote(
            relays[w].at[:, along_z(k)], target, z_leg_send.at[w, k], z_leg_recv.at[w, k],
            {"dp": y * NZ + along_z(k)},
        )

    def straight(p, k):
        q, first, width = STRAIGHT[p]
        source = (send_r, send_a)[q].at[y * NZ + along_z(k), :, pl.ds(first * unit, width * unit)]
        return remote(
            source, (recv_r, recv_a, last)[p].at[0, z], a_send.at[p, k], a_recv.at[p, k],
            {"dp": y * NZ + along_z(k)},
        )

    def start_y_leg(w):
        for j in range(1, n_y):
            y_leg(w, j).start()

    def start_straight(p):
        for k in STEPS:
            straight(p, k).start()

    def forward(w):
        for j in range(1, n_y):
            y_leg(w, j).wait_recv()
        if w == final:
            for place in PLANES:
                k = lax.rem(place - z + NZ, NZ)

                @pl.when(k != 0)
                def _():
                    z_leg(w, k).start()
        else:
            for k in STEPS:
                z_leg(w, k).start()
        q, first, width = CHUNKS[w]
        for j in range(1, n_y):
            if w == final:
                last[j, z] = relays[w][j - 1, z]
            else:
                (recv_r, recv_a)[q][j, z, :, first * unit : (first + width) * unit] = relays[w][j - 1, z]

    start_y_leg(0)
    start_straight(0)
    start_y_leg(1)
    start_y_leg(2)

    for b in range(2):
        for q, ref in enumerate((len_ref, rate_ref)):
            spread = jnp.broadcast_to(column(ref[b : b + 1, :].astype(F32)), (LANES, LANES))
            per = LANES // piece
            cols[q, per * b : per * (b + 1)] = spread.reshape(per, piece, LANES)

    for i in range(4):
        load(1, i).wait()

    def gather_v(d, c):
        p = slots_ref[d]
        vals[d] = vbuf[p]
        sums[0, d] = cols[0, p]
        sums[1, d] = cols[1, p]
        return c

    lax.fori_loop(0, n_dp, gather_v, 0)
    recv_r[0, z] = send_r[me]

    lane = iota((rows, LANES), 1)
    lane_f = lane.astype(F32)
    lengths = sums[0].reshape(rows, LANES).astype(jnp.int32)
    rate = sums[1].reshape(rows, LANES)
    cols[0] = sums[0]
    scales[0] = jnp.exp(-rate)
    scales[1] = jnp.exp(-rate * lane_f)
    scales[2] = jnp.exp(rate * lane_f)
    scales[3] = jnp.exp(-rate * (LANES - lane_f))
    sums[...] = jnp.zeros_like(sums)
    triangle = (iota((LANES, LANES), 0) >= iota((LANES, LANES), 1)).astype(F32)

    def block(i, carry):
        next_head, next_value = carry
        at = span // LANES - 1 - i
        lanes = pl.ds(pl.multiple_of(at * LANES, LANES), LANES)
        position = at * LANES + lane
        length = cols[0].reshape(rows, LANES).astype(jnp.int32)
        reward = send_r[:, :, lanes].astype(F32).reshape(rows, LANES)
        value = vals[:, :, lanes].astype(F32).reshape(rows, LANES)
        valid = position < length
        value_next = jnp.where(lane == LANES - 1, next_value, pltpu.roll(value, LANES - 1, 1))
        value_next = jnp.where(position + 1 < length, value_next, 0.0)
        td = jnp.where(valid, reward + scales[0] * value_next - value, 0.0)
        local = dot(td * scales[1], triangle, precision=HIGHEST) * scales[2]
        total = local + scales[3] * next_head
        rounded = jnp.where(valid, total, 0.0).astype(BF16)
        send_a[:, :, lanes] = rounded.reshape(n_dp, piece, LANES)
        reward = jnp.where(valid, reward, 0.0)
        kept = rounded.astype(F32)
        for q, term in enumerate((reward, kept, reward * reward, kept * kept)):
            sums[q] += term.reshape(n_dp, piece, LANES)
        return total[:, 0:1], value[:, 0:1]

    zero = jnp.zeros((rows, 1), F32)
    third = span // LANES // 3
    carry = lax.fori_loop(0, third, block, (zero, zero))
    forward(0)
    carry = lax.fori_loop(third, 2 * third, block, carry)
    forward(1)
    lax.fori_loop(2 * third, span // LANES, block, carry)
    recv_a[0, z] = send_a[me, :, 0 : span // 2]
    last[0, z] = send_a[me, :, span // 2 : span]

    term_of, row_of = lane // piece, lax.rem(lane, piece)
    own = row_of == lax.rem(iota((rows, LANES), 0), piece)
    packed = jnp.where(own & (term_of == 0), cols[0].reshape(rows, LANES), 0.0)
    for q in range(4):
        total = jnp.sum(sums[q].reshape(rows, LANES), axis=1, keepdims=True)
        packed = jnp.where(own & (term_of == q + 1), total, packed)
    tsend[...] = jnp.sum(packed.reshape(n_dp, piece, LANES), axis=1, keepdims=True)

    for b in range(2):
        here = slice(b * LANES, (b + 1) * LANES)
        order = column(perm_ref[b : b + 1, :].astype(F32)).astype(jnp.int32)
        chooser[b] = (order == iota((LANES, LANES), 1)).astype(BF16)
        batch = column(batch_ref[b : b + 1, :].astype(F32)).astype(jnp.int32)
        member[here] = (batch == iota((LANES, LANES), 1)).astype(F32)

    def terms_y(j):
        return remote(
            tsend.at[pl.ds(along_y(j) * NZ, NZ)], trelay.at[j], t1_send.at[j], t1_recv.at[j],
            {"dp": along_y(j) * NZ + z},
        )

    def terms_z(k):
        return remote(
            trelay.at[:, along_z(k)], trecv.at[:, z], t2_send.at[k], t2_recv.at[k],
            {"dp": y * NZ + along_z(k)},
        )

    trelay[0] = tsend[pl.ds(y * NZ, NZ)]
    for j in range(1, n_y):
        terms_y(j).start()
    start_y_leg(3)
    start_y_leg(4)
    for j in range(1, n_y):
        terms_y(j).wait()
    for k in STEPS:
        terms_z(k).start()
    forward(2)
    trecv[:, z] = trelay[:, z]
    for k in STEPS:
        terms_z(k).wait()

    ordered = [trecv[lax.rem(y - h + n_y, n_y)] for h in range(n_y)]
    spread = jnp.concatenate(ordered, axis=0)
    spread = jnp.broadcast_to(spread, (n_dp, piece, LANES)).reshape(rows, LANES)
    spread = jnp.where(own, spread, 0.0)
    select = (iota((LANES, LANES), 0) // piece == iota((LANES, LANES), 1)).astype(F32)
    totals = jnp.zeros((LANES, LANES), F32)
    for b in range(2):
        here = slice(b * LANES, (b + 1) * LANES)
        moved = dot(chooser[b].astype(F32), spread[here], precision=HIGHEST)
        moved = dot(moved, select, precision=HIGHEST)
        stats[2, here] = jnp.broadcast_to(moved[:, 0:1], (LANES, LANES))
        totals += dot(moved, member[here], (((0,), (0,)), ((), ())), precision=HIGHEST)

    def exchange(store, index, sizes, target, send_sem, recv_sem, between):
        store[index] = part[...]

        def copy(k):
            return pltpu.make_async_remote_copy(
                part, store.at[index], send_sem.at[k], recv_sem.at[k],
                device_id=target(k), device_id_type=MESH,
            )

        def go(k, c):
            copy(k).start()
            return c

        def done(k, c):
            copy(k).wait()
            return c

        lax.fori_loop(1, sizes, go, 0)
        between()
        lax.fori_loop(1, sizes, done, 0)
        part[...] = jnp.sum(store[...], axis=0)

    part[...] = totals[0:8]
    exchange(
        st_g, group, n_group, lambda k: {"group": lax.rem(group + k, n_group)},
        g_send, g_recv, lambda: None,
    )
    def advantage_straight():
        start_straight(1)
        start_straight(2)
        forward(3)

    exchange(
        st_z, z, NZ, lambda k: {"dp": y * NZ + along_z(k)}, z_send, z_recv, advantage_straight
    )
    exchange(
        st_y, y, n_y, lambda k: {"dp": along_y(k) * NZ + z}, y_send, y_recv, lambda: forward(final)
    )

    total = part[...]
    count = jnp.maximum(total[0:1], 1.0)
    for q in range(2):
        mean = total[1 + q : 2 + q] / count
        spread = jnp.maximum(total[3 + q : 4 + q] / count - mean * mean, 0.0)
        for s, value in enumerate((mean, lax.rsqrt(spread + 1e-05))):
            picked = jnp.sum(member[...] * value, axis=1, keepdims=True)
            (stats_r, stats)[q][s] = jnp.broadcast_to(picked, (rows, LANES))

    tile = 256
    for w, (q, first, width) in enumerate(CHUNKS):
        if w == final:
            for c in range(len(CHUNKS)):
                for j in range(1, n_y):
                    y_leg(c, j).wait_send()
        for p, (kind, begin, _) in enumerate(STRAIGHT):
            if (kind, begin) == (q, first):
                for k in STEPS:
                    straight(p, k).wait()
        for k in STEPS:
            z_leg(w, k).wait()
        if w == final:
            break
        source, out, moments = ((recv_r, out_r, stats_r), (recv_a, out_a, stats))[q]

        def finish(i, c):
            start = pl.multiple_of(first * unit + i * tile, LANES)
            for b in range(2):
                here = slice(b * LANES, (b + 1) * LANES)
                out[here, pl.ds(start, tile)] = whiten(
                    source, y, b, pl.ds(start, tile), chooser[b],
                    moments[0, here], moments[1, here], stats[2, here].astype(jnp.int32), start,
                )
            return c

        lax.fori_loop(0, width * unit // tile, finish, 0)


def finish_kernel(n_dp, white_r, white_a, last, chooser, stats, out_r, out_a, white, sem):
    rows, width = white.shape
    ready = white_a.shape[1]
    y = lax.axis_index("dp") // NZ
    copies = []

    def send(source, target):
        copy = pltpu.make_async_copy(source, target, sem.at[len(copies)])
        copy.start()
        copies.append(copy)

    for i in range(4):
        here = pl.ds(i * (rows // 4), rows // 4)
        send(white_r.at[here], out_r.at[here])
        send(white_a.at[here], out_a.at[here, 0:ready])
    tile = 512
    for i in range(width // tile):
        lanes = slice(i * tile, (i + 1) * tile)
        for b in range(2):
            here = slice(b * LANES, (b + 1) * LANES)
            white[here, lanes] = whiten(
                last, y, b, lanes, chooser[b],
                stats[0, here], stats[1, here], stats[2, here].astype(jnp.int32), ready + i * tile,
            )
        send(white.at[:, lanes], out_a.at[:, ready + i * tile : ready + (i + 1) * tile])
    for copy in copies:
        copy.wait()


def local(rewards, values, lengths, decay_rate, piece_dest, row_perm, minibatch, *, n_dp, n_group):
    rows, span = rewards.shape
    piece = rows // n_dp
    half = span // 2
    unit = span // 4
    n_y = n_dp // NZ
    vmem = pl.BlockSpec(memory_space=pltpu.VMEM)
    hbm = pl.BlockSpec(memory_space=pltpu.HBM)
    bulk = pltpu.VMEM((n_dp, piece, span), BF16)
    dma = pltpu.SemaphoreType.DMA
    chunks = len(CHUNKS)
    result = jax.ShapeDtypeStruct((rows, span), BF16)
    parts = pl.pallas_call(
        functools.partial(kernel, (n_dp, n_group, piece, span)),
        out_shape=(
            result,
            jax.ShapeDtypeStruct((rows, half), BF16),
            jax.ShapeDtypeStruct((n_y, NZ, piece, half), BF16),
            jax.ShapeDtypeStruct((2, LANES, LANES), BF16),
            jax.ShapeDtypeStruct((3, rows, LANES), F32),
        ),
        in_specs=[hbm] * 7,
        out_specs=(vmem,) * 5,
        scratch_shapes=[
            pltpu.SMEM((1, n_dp), jnp.int32),
            pltpu.SMEM((n_dp,), jnp.int32),
            pltpu.VMEM((2, LANES), jnp.int32),
            pltpu.VMEM((2, LANES), F32),
            pltpu.VMEM((2, LANES), jnp.int32),
            pltpu.VMEM((2, LANES), jnp.int32),
        ]
        + [bulk] * 5
        + [
            pltpu.VMEM((n_y, NZ, piece, span), BF16),
            pltpu.VMEM((n_y, NZ, piece, half), BF16),
        ]
        + [pltpu.VMEM((n_y - 1, NZ, piece, w * unit), BF16) for _, _, w in CHUNKS]
        + [
            pltpu.VMEM((2, n_dp, piece, LANES), F32),
            pltpu.VMEM((4, rows, LANES), F32),
            pltpu.VMEM((4, n_dp, piece, LANES), F32),
            pltpu.VMEM((rows, LANES), F32),
            pltpu.VMEM((2, rows, LANES), F32),
            pltpu.VMEM((n_dp, 1, LANES), F32),
            pltpu.VMEM((n_y, NZ, 1, LANES), F32),
            pltpu.VMEM((n_y, NZ, 1, LANES), F32),
            pltpu.VMEM((8, LANES), F32),
            pltpu.VMEM((NZ, 8, LANES), F32),
            pltpu.VMEM((n_y, 8, LANES), F32),
            pltpu.VMEM((n_group, 8, LANES), F32),
            dma((13,)),
            dma((chunks, n_y)), dma((chunks, n_y)),
            dma((chunks, NZ)), dma((chunks, NZ)),
            dma((len(STRAIGHT), NZ)), dma((len(STRAIGHT), NZ)),
            dma((n_y,)), dma((n_y,)),
            dma((NZ,)), dma((NZ,)),
            dma((n_group,)), dma((n_group,)),
            dma((NZ,)), dma((NZ,)),
            dma((n_y,)), dma((n_y,)),
        ],
        compiler_params=pltpu.CompilerParams(
            collective_id=0, has_side_effects=True, vmem_limit_bytes=40 * 2**20
        ),
        name="reshuffle",
    )(
        *(
            pltpu.with_memory_space_constraint(array, pltpu.HBM)
            for array in (
                piece_dest,
                lengths.reshape(2, LANES),
                decay_rate.reshape(2, LANES),
                minibatch.reshape(2, LANES),
                row_perm,
                rewards.reshape(n_dp, piece, span),
                values.reshape(n_dp, piece, span),
            )
        )
    )
    return pl.pallas_call(
        functools.partial(finish_kernel, n_dp),
        out_shape=(result, result),
        in_specs=[vmem] * 5,
        out_specs=(hbm, hbm),
        scratch_shapes=[pltpu.VMEM((rows, half), BF16), dma((12,))],
        compiler_params=pltpu.CompilerParams(vmem_limit_bytes=16 * 2**20),
        name="finish",
    )(*parts)


def solution(mesh):
    both = ("dp", "group")
    return jax.shard_map(
        functools.partial(local, n_dp=mesh.shape["dp"], n_group=mesh.shape["group"]),
        mesh=mesh,
        in_specs=(
            P(both, None), P(both, None), P(both), P(both), P("dp", None), P(both, None), P(both),
        ),
        out_specs=(P(both, None), P(both, None)),
        check_vma=False,
    )
```
